32 devices in a mesh: gx: 4 (over y, core), gy: 8 (over z, x).
Axes of the slice: x: 2, y: 2, z: 4, core: 2. Of those that a mesh axis runs over, the one named last changes fastest.
Arguments:
- thermal_anomaly: float32 [32, 128, 1024], P(None, 'gx', 'gy'), may hold values from -6 to 6
- ambient_diffusion: bfloat16 [128, 1024], P('gx', 'gy'), may hold values from 0.019897461 to 0.25
- solar_light: bfloat16 [128, 1024], P('gx', 'gy'), may hold values from 0.5 to 4
- sea_tile_flags: int32 [4, 8, 64], P('gx', 'gy'), may hold values 0 or 1
- flooded_layer_tally: int32 [4, 8, 64], P('gx', 'gy'), may hold values from 1 to 32
- tile_holder_rank: int32 [4, 8, 64, 1], P('gx', 'gy'), may hold values from 0 to 7; in each aligned block of 64 rows (0 to 63, 64 to 127, ..., all dimensions but the last counted through in order) at most 16 rows name the same one
- solute_amounts: float32 [4, 8, 128, 8, 2048], P('gx', 'gy'), may hold values from 0.09 to 11
- reaction_rates: float32 [8, 8], replicated, may hold values from -0.2 to 0.5
Outputs:
- thermal_final: float32 [32, 128, 1024], P(None, 'gx', 'gy')
- solute_final: float32 [4, 8, 128, 8, 2048], P('gx', 'gy')
The draws below stay inside these ranges and needn't reach their ends.
Inputs may be any that keep to these rules, and one draw needn't show every extreme that they name: `tile_holder_rank`: among the 64 blocks of one device, at most 16 name the same owner, a bound that some block reaches of them.
All inputs are finite; a program needn't handle non-finite values. No bound on the sum of `sea_tile_flags` on one device may be relied on, other than what follows from the above.
Results may differ from the reference program's by a relative error of at most 0.0003.
Values may be sent and summed in bfloat16 or wider, within the bound.
No kernel may reach another device: no remote copies, remote signals or barrier semaphores. Data moves between devices by JAX's collectives and lax.ppermute only.
A program may use at most 128 MiB of HBM per device.

```python
import math
import jax
import jax.numpy as jnp
import numpy as np
from jax import lax

VERTICAL_LAYERS = 32
TRACER_COUNT = 8
TILES_EAST = 4
TILES_NORTH = 16
GRID_WIDTH_EAST = 128
GRID_WIDTH_NORTH = 1024
SLOT_CAPACITY = 16
SLOTS = 128
LCOL = 2048
N_GX = 4
N_GY = 8


def draw_solute_amounts(key, part):
    key_level = jax.random.fold_in(key, 11)
    key_cells = jax.random.fold_in(key, 12)
    device_total = N_GX * N_GY
    flat_index = (lax.broadcasted_iota(jnp.int32, (N_GX, N_GY, 1, 1, 1), 0) * N_GY + lax.broadcasted_iota(jnp.int32, (N_GX, N_GY, 1, 1, 1), 1)).astype(jnp.float32)
    ramp_pos = flat_index / float(max(device_total - 1, 1)) - 0.5
    full_shape = (N_GX, N_GY, SLOTS, TRACER_COUNT, LCOL)
    level_noise = jax.random.uniform(key_level, (N_GX, N_GY, 1, TRACER_COUNT, 1), jnp.float32, -0.7, 0.7)
    dev_level = jnp.exp(level_noise + math.log(3.0) * ramp_pos)
    cell_factor = jnp.exp(jax.random.uniform(key_cells, full_shape, jnp.float32, math.log(0.5), math.log(2.0)))
    return dev_level * cell_factor


def touch_ends(entries, key, least, top_value):
    longest = entries.shape.index(max(entries.shape))
    spots = []
    for shift in (0, 1):
        where = [jax.random.randint(jax.random.fold_in(key, axis), (), 0, length) for axis, length in enumerate(entries.shape)]
        where[longest] = (where[longest] + shift) % entries.shape[longest]
        spots.append(tuple(where))
    return entries.at[spots[0]].set(least).at[spots[1]].set(top_value)


def shard_levels(key, dims, shards, low, top_value):
    def one(position, parts):
        heights = jax.random.uniform(jax.random.fold_in(jax.random.fold_in(key, 6), position), (parts,), jnp.float32, low / len(shards), top_value / len(shards))
        return jnp.repeat(jnp.exp(heights), dims[position] // parts).reshape((-1,) + (1,) * (len(dims) - position - 1))

    level = one(*shards[0])
    for cut in shards[1:]:
        level = level * one(*cut)
    return level


def shared_out(stream_key, own, number, rows, count, top, reach, lean):
    order = jax.random.permutation(stream_key, count)
    heavy_load, ordinary = portions_of(count, rows * top, reach, lean, True), portions_of(count, rows * top, reach, lean, False)
    places = jnp.arange(count)

    def named(tallies, turn):
        used = int((tallies > 0).sum())
        fixed = max(1, used // 4)
        shifted = fixed + (places - fixed + turn * (used - fixed)) % max(1, count - fixed)
        return jnp.zeros((count,), jnp.int32).at[order[jnp.where(places < fixed, places, shifted)]].set(jnp.asarray(tallies, jnp.int32))

    tallies = jnp.where(number % 4 == 0, named(heavy_load, number // 4), named(ordinary, number - number // 4 - 1))
    mixed = jax.random.permutation(jax.random.fold_in(own, 3), count)
    source_of, taker = mixed[0:count // 2 * 2:2], mixed[1:count // 2 * 2:2]
    margin = jnp.minimum(tallies[source_of] - 1, reach - tallies[taker]) // 2
    margin = jnp.where((source_of == order[0]) | (taker == order[0]) | (tallies[taker] == 0), 0, jnp.maximum(margin, 0))
    shifted = jax.random.randint(jax.random.fold_in(own, 4), (count // 2,), 0, 1 << 20) % (margin + 1)
    tallies = tallies.at[source_of].add(-shifted).at[taker].add(shifted)
    labels = jnp.searchsorted(jnp.cumsum(tallies), jnp.arange(rows * top), side="right").astype(jnp.int32)
    listing = labels.reshape(top, rows).T
    listing = listing[jax.random.permutation(jax.random.fold_in(own, 1), rows)]
    turn = jax.random.randint(jax.random.fold_in(own, 2), (rows, 1), 0, top)
    return jnp.take_along_axis(listing, (jnp.arange(top)[None, :] + turn) % top, axis=1)


def portions_of(count, total, limit, lean, full):
    weights = [(1 << 20) // math.isqrt(grade ** lean) + 1 for grade in range(1, count + 1)]
    largest = limit if full else min(limit, max(-(-total // count), total * weights[0] // sum(weights)))
    least = 1 if total - largest >= count - 1 else 0
    counts, spare = [largest] + [least] * (count - 1), total - largest - least * (count - 1)
    while spare > 0:
        movable = [i for i in range(1, count) if counts[i] < largest] or [i for i in range(1, count) if counts[i] < limit]
        whole, remaining = sum([weights[i] for i in movable]), spare
        for i in movable:
            addition = min(limit - counts[i], max(1, remaining * weights[i] // whole), spare)
            counts[i] = counts[i] + addition
            spare = spare - addition
    return np.array(counts)


def normal_values(own_key, dims, scale, bound, pieces=(), held_as=jnp.bfloat16):
    loudness = shard_levels(own_key, dims, pieces, -0.22, 0.18) if pieces else 1.0
    result = jax.random.normal(own_key, dims, jnp.float32) * scale * loudness
    return jnp.minimum(jnp.maximum(result, -bound), bound).astype(held_as)


def setup_inputs(seed: int = 0) -> dict:
    key_list = jax.random.split(jax.random.key(seed), 9)
    thermal_anomaly = normal_values(key_list[0], (VERTICAL_LAYERS, GRID_WIDTH_EAST, GRID_WIDTH_NORTH), 1.0, 6.0, ((1, 4), (2, 8)), jnp.float32)
    ambient_diffusion = jnp.clip(jnp.exp(math.log(0.25) - 2.5308688 * jax.random.uniform(key_list[1], (GRID_WIDTH_EAST, GRID_WIDTH_NORTH), jnp.float32) ** shard_levels(key_list[1], (GRID_WIDTH_EAST, GRID_WIDTH_NORTH), ((0, 4), (1, 8)), -0.2, 0.2)), 0.019897461, 0.25).astype(jnp.bfloat16)
    solar_light = jnp.clip(jnp.exp(math.log(4.0) - 2.0794415 * jax.random.uniform(key_list[2], (GRID_WIDTH_EAST, GRID_WIDTH_NORTH), jnp.float32) ** shard_levels(key_list[2], (GRID_WIDTH_EAST, GRID_WIDTH_NORTH), ((0, 4), (1, 8)), -0.2, 0.2)), 0.5, 4.0).astype(jnp.bfloat16)
    sea_tile_flags = touch_ends((jax.random.randint(key_list[3], (N_GX, N_GY, TILES_EAST * TILES_NORTH), 0, 8) < 7).astype(jnp.int32), jax.random.fold_in(key_list[3], 1), 0, 1)
    flooded_layer_tally = touch_ends(jax.random.randint(key_list[4], (N_GX, N_GY, TILES_EAST * TILES_NORTH), 1, VERTICAL_LAYERS + 1), jax.random.fold_in(key_list[4], 1), 1, VERTICAL_LAYERS).astype(jnp.int32)
    tile_holder_rank_keys = jax.random.split(jax.random.fold_in(key_list[5], 1), N_GX * N_GY * (TILES_EAST * TILES_NORTH) // (TILES_EAST * TILES_NORTH))
    tile_holder_rank_turns = jax.random.permutation(jax.random.fold_in(key_list[5], 3), N_GX * N_GY * (TILES_EAST * TILES_NORTH) // (TILES_EAST * TILES_NORTH))
    tile_holder_rank = jax.vmap(lambda own, number: shared_out(jax.random.fold_in(key_list[5], 2), own, number, TILES_EAST * TILES_NORTH, N_GY, 1, SLOT_CAPACITY, 2))(tile_holder_rank_keys, tile_holder_rank_turns).reshape((N_GX, N_GY, TILES_EAST * TILES_NORTH, 1))
    solute_amounts = draw_solute_amounts(jax.random.fold_in(key_list[8], 71), 0)
    reaction_rates = jnp.clip(jax.random.uniform(key_list[7], (TRACER_COUNT, TRACER_COUNT), jnp.float32, -0.2, 0.5), -0.2, 0.5)
    return dict(thermal_anomaly=thermal_anomaly, ambient_diffusion=ambient_diffusion, solar_light=solar_light, sea_tile_flags=sea_tile_flags, flooded_layer_tally=flooded_layer_tally, tile_holder_rank=tile_holder_rank, solute_amounts=solute_amounts, reaction_rates=reaction_rates)


NU_COEF = 0.2
STEP_DT = 0.05
ATTEN_WATER = 0.06
ATTEN_CHL = 0.05
WARMING_SCALE = 0.5
GROWTH_TEMP = 0.063


def masked_step(field, within_layer):
    center = field[:, 1:-1, 1:-1]
    span_east = center.shape[1]
    span_north = center.shape[2]
    total = jnp.zeros_like(center)
    for first, second in ((0, 1), (2, 1), (1, 0), (1, 2)):
        near = field[:, first:first + span_east, second:second + span_north]
        total = total + within_layer[:, first:first + span_east, second:second + span_north] * (near - center)
    return center + NU_COEF * within_layer[:, 1:-1, 1:-1] * total


def diffusion_mixer(temp_b, kbg_b):
    below = jnp.concatenate([temp_b[..., 1:, :], temp_b[..., -1:, :]], axis=-2)
    return (kbg_b[..., None, :] * (1.0 + 0.5 * jnp.tanh(temp_b - below))).astype(jnp.bfloat16)


def validity(tile_amount):
    levels = lax.broadcasted_iota(jnp.int32, (1, VERTICAL_LAYERS, 1), 1)
    valid = (levels < tile_amount[:, None, None]).astype(jnp.float32)
    active = (levels + 1 < tile_amount[:, None, None]).astype(jnp.float32)
    return valid, active


def totals(amounts_on_chip, valid):
    return jnp.sum(amounts_on_chip * valid[:, None], axis=(0, 2, 3))


def column_step(temp_b, kappa_b, sw_b, tile_amount, amounts_on_chip, reaction_rates):
    valid, active = validity(tile_amount)
    atten = ATTEN_WATER + ATTEN_CHL * amounts_on_chip[:, 0]
    cumul = jnp.cumsum(atten, axis=1)
    surface = sw_b.astype(jnp.float32)[:, None, :]
    top = surface * jnp.exp(-(cumul - atten))
    bottom = surface * jnp.exp(-cumul)
    heat = (valid * (top - bottom)).astype(jnp.bfloat16)
    growth = jnp.exp(GROWTH_TEMP * temp_b.astype(jnp.float32)) * top / (top + 1.0)
    mixed = jnp.einsum("rs,nslc->nrlc", reaction_rates, amounts_on_chip, precision=lax.Precision.HIGHEST)
    below = jnp.concatenate([amounts_on_chip[:, :, 1:], amounts_on_chip[:, :, -1:]], axis=2)
    flux = (kappa_b.astype(jnp.float32) * active)[:, None] * (below - amounts_on_chip)
    above = jnp.concatenate([jnp.zeros_like(flux[:, :, :1]), flux[:, :, :-1]], axis=2)
    new = amounts_on_chip + valid[:, None] * STEP_DT * (flux - above + growth[:, None] * mixed)
    return new, heat


def cells_of(per_block):
    grid = per_block.reshape(N_GX, N_GY, TILES_EAST, TILES_NORTH).transpose(0, 2, 1, 3).reshape(N_GX * TILES_EAST, N_GY * TILES_NORTH)
    return jnp.repeat(jnp.repeat(grid, 8, axis=0), 8, axis=1)


def blocks_2d(field):
    return field.reshape(N_GX, TILES_EAST, 8, N_GY, TILES_NORTH, 8).transpose(0, 3, 1, 4, 2, 5).reshape(N_GX, N_GY, TILES_EAST * TILES_NORTH, 64)


def reference(thermal_anomaly, ambient_diffusion, solar_light, sea_tile_flags, flooded_layer_tally, tile_holder_rank, solute_amounts, reaction_rates):
    depth_block = sea_tile_flags * flooded_layer_tally
    cell_count = cells_of(depth_block)
    level_idx = lax.broadcasted_iota(jnp.int32, (VERTICAL_LAYERS, 1, 1), 0)
    within_layer = (level_idx < cell_count[None]).astype(jnp.float32)
    piled_tiles = jnp.pad(jnp.stack([thermal_anomaly, within_layer]), ((0, 0), (0, 0), (1, 1), (1, 1)))
    advanced_verticals = masked_step(piled_tiles[0], piled_tiles[1])
    dispatched = advanced_verticals.astype(jnp.bfloat16)
    thermal_tiles = dispatched.reshape(VERTICAL_LAYERS, N_GX, TILES_EAST, 8, N_GY, TILES_NORTH, 8).transpose(1, 4, 2, 5, 0, 3, 6).reshape(N_GX, N_GY, TILES_EAST * TILES_NORTH, VERTICAL_LAYERS, 64)
    ambient_diffusion_tiles = blocks_2d(ambient_diffusion)
    shortwave_blocks = blocks_2d(solar_light)
    diffusion_each_tile = diffusion_mixer(thermal_tiles.astype(jnp.float32), ambient_diffusion_tiles.astype(jnp.float32))
    holder_chip = tile_holder_rank[..., 0]
    order = jnp.arange(TILES_EAST * TILES_NORTH, dtype=jnp.int32)
    same = (holder_chip[..., :, None] == holder_chip[..., None, :]) & (order[None, :] < order[:, None])
    rank = jnp.sum(same.astype(jnp.int32), axis=-1)
    position_rank = (jnp.arange(N_GY, dtype=jnp.int32)[None, :, None] * SLOT_CAPACITY + rank).astype(jnp.int32)
    tile_line = jnp.broadcast_to(jnp.arange(N_GX, dtype=jnp.int32)[:, None, None], holder_chip.shape)
    position_summation = N_GY * SLOT_CAPACITY
    compact_warmth = jnp.zeros((N_GX, N_GY, position_summation, VERTICAL_LAYERS, 64), jnp.bfloat16).at[tile_line, holder_chip, position_rank].set(thermal_tiles)
    compact_diffusion = jnp.zeros((N_GX, N_GY, position_summation, VERTICAL_LAYERS, 64), jnp.bfloat16).at[tile_line, holder_chip, position_rank].set(diffusion_each_tile)
    packed_shortwave = jnp.zeros((N_GX, N_GY, position_summation, 64), jnp.bfloat16).at[tile_line, holder_chip, position_rank].set(shortwave_blocks)
    packed_level_count = jnp.zeros((N_GX, N_GY, position_summation), jnp.int32).at[tile_line, holder_chip, position_rank].set(depth_block)
    concentration_global = solute_amounts.reshape(N_GX, N_GY * position_summation, TRACER_COUNT, VERTICAL_LAYERS, 64)

    def owner_pass(items):
        temp_b, kappa_b, sw_b, tile_amount, amounts_on_chip = items
        valid, active = validity(tile_amount)
        new, heat = column_step(temp_b, kappa_b, sw_b, tile_amount, amounts_on_chip, reaction_rates)
        return new, heat, totals(amounts_on_chip, valid), totals(new, valid), jnp.sum(valid) * 64.0

    updated_global, heat_global, old_parts, new_parts, cell_parts = lax.map(owner_pass, (
        compact_warmth.reshape(N_GX, N_GY * position_summation, VERTICAL_LAYERS, 64), compact_diffusion.reshape(N_GX, N_GY * position_summation, VERTICAL_LAYERS, 64),
        packed_shortwave.reshape(N_GX, N_GY * position_summation, 64), packed_level_count.reshape(N_GX, N_GY * position_summation), concentration_global))
    old_total = jnp.sum(old_parts, axis=0)
    new_total = jnp.sum(new_parts, axis=0)
    cells = jnp.sum(cell_parts)
    shift = (old_total - new_total) / jnp.maximum(cells, 1.0)

    def totals_corrected(items):
        new, amounts_on_chip, tile_amount = items
        valid, active = validity(tile_amount)
        return jnp.where(valid[:, None] > 0, new + shift[None, :, None, None], amounts_on_chip)

    solute_final = lax.map(totals_corrected, (updated_global, concentration_global, packed_level_count.reshape(N_GX, N_GY * position_summation)))
    solute_final = solute_final.reshape(solute_amounts.shape)
    heat_in_slots = heat_global.reshape(N_GX, N_GY, position_summation, VERTICAL_LAYERS, 64)
    heat_blocks = heat_in_slots[tile_line, holder_chip, position_rank]
    warming_each_site = heat_blocks.reshape(N_GX, N_GY, TILES_EAST, TILES_NORTH, VERTICAL_LAYERS, 8, 8).transpose(4, 0, 2, 5, 1, 3, 6).reshape(VERTICAL_LAYERS, N_GX * TILES_EAST * 8, N_GY * TILES_NORTH * 8)
    thermal_final = advanced_verticals + WARMING_SCALE * warming_each_site.astype(jnp.float32)
    return thermal_final, solute_final
```

```python
import functools
import jax
import jax.numpy as jnp
from jax import lax
from jax.experimental import pallas as pl
from jax.experimental.pallas import tpu as pltpu
from jax.sharding import PartitionSpec as P

NU_COEF = 0.2
STEP_DT = 0.05
ATTEN_WATER = 0.06
ATTEN_CHL = 0.05
WARMING_SCALE = 0.5
GROWTH_TEMP = 0.063
LANES = 128
HALF = 64
SUB = 8


f32 = jnp.float32
bf16 = jnp.bfloat16


def iota(shape, dim):
    return lax.broadcasted_iota(jnp.int32, shape, dim)


def swap_granules(x):
    row = iota(x.shape, 1)
    lane = iota(x.shape, 2)
    for step in (1, 2, 4):
        r = (row & step) != 0
        c = (lane & (step * SUB)) != 0
        w = step * SUB
        up = pltpu.roll(pltpu.roll(x, SUB - step, 1), w, 2)
        down = pltpu.roll(pltpu.roll(x, step, 1), LANES - w, 2)
        x = jnp.where(r == c, x, jnp.where(c, up, down))
    return x


def join_levels(a, b):
    low = iota(a.shape, 2) < HALF
    return (
        jnp.where(low, a, pltpu.roll(b, HALF, 2)),
        jnp.where(low, pltpu.roll(a, HALF, 2), b),
    )


def row_of(ref, *at, n=SUB):
    return ref[(*at[:-1], pl.ds(at[-1], n, stride=0), slice(None))]


def depth_rows(depth, blocks_y):
    n = depth.shape[1]
    mine = iota((SUB, n), 1) // blocks_y == iota((SUB, n), 0)
    left = jnp.where(mine, jnp.broadcast_to(depth, (SUB, n)), 0.0)
    spread = iota((n, LANES), 0) % blocks_y == iota((n, LANES), 1) // SUB
    return jnp.dot(left, spread.astype(f32), preferred_element_type=f32)


def edge_depth(depth, blocks_x, blocks_y, by):
    n = depth.shape[1]
    pick = iota((n, LANES), 0) == (iota((n, LANES), 1) % blocks_x) * blocks_y + by
    return jnp.dot(
        jnp.broadcast_to(depth, (SUB, n)), pick.astype(f32), preferred_element_type=f32
    )


def edges_kernel(bx_n, by_n, *refs):
    sources, (xlo, xhi, ylo, yhi), held, sems = refs[:6], refs[6:10], refs[10:16], refs[16]
    t, flags, tally = held[:3]
    levels, nx, _ = t.shape
    loads = [
        pltpu.make_async_copy(x, y, sems.at[i]) for i, (x, y) in enumerate(zip(sources, held))
    ]
    for load in loads:
        load.start()
    for load in loads:
        load.wait()
    depth = (flags[...] * tally[...]).astype(f32)
    d = depth_rows(depth, by_n)
    for k in range(levels):
        xlo[k : k + 1, :] = t[k, 0:1, :]
        xhi[k : k + 1, :] = t[k, nx - 1 : nx, :]
    xlo[levels : levels + SUB, :] = jnp.broadcast_to(d[0:1], (SUB, LANES))
    xhi[levels : levels + SUB, :] = jnp.broadcast_to(d[bx_n - 1 : bx_n], (SUB, LANES))
    lane = iota((SUB, LANES), 1)
    lo = jnp.zeros((SUB, LANES), f32)
    hi = jnp.zeros((SUB, LANES), f32)
    for k0 in range(0, levels, 4):
        places = [(k, bx) for k in range(k0, k0 + 4) for bx in range(bx_n)]
        tiles = [t[k, bx * SUB : (bx + 1) * SUB, :] for k, bx in places]
        js = [k * bx_n + bx for k, bx in places]
        los = [pltpu.roll(v, j, 1) for v, j in zip(tiles, js)]
        his = [pltpu.roll(v, (j + 1) % LANES, 1) for v, j in zip(tiles, js)]
        for j, a, b in zip(js, los, his):
            lo = jnp.where(lane == j, a, lo)
            hi = jnp.where(lane == j, b, hi)
    ylo[0:SUB, :] = lo
    yhi[0:SUB, :] = hi
    k_lane = (lane // bx_n).astype(f32)
    ylo[SUB:, :] = (k_lane < edge_depth(depth, bx_n, by_n, 0)).astype(f32)
    yhi[SUB:, :] = (k_lane < edge_depth(depth, bx_n, by_n, by_n - 1)).astype(f32)


def slots_kernel(bx_n, by_n, cap, n_gy, amb, light, flags, tally, holder, sel, sel_t, tail):
    n = bx_n * by_n
    slots = sel.shape[0]
    me = lax.axis_index("gy").astype(f32)
    own = holder[...].astype(f32)
    row_i = iota((n, n), 0)
    col_i = iota((n, n), 1)
    own_row = jnp.broadcast_to(own, (n, n))
    own_col = jnp.sum(jnp.where(row_i == col_i, own_row, 0.0), axis=1, keepdims=True)
    same = own_row == own_col
    rank_row = jnp.sum(jnp.where(same & (row_i < col_i), 1.0, 0.0), axis=0, keepdims=True)
    rank_col = jnp.sum(jnp.where(same & (col_i < row_i), 1.0, 0.0), axis=1, keepdims=True)
    to_row = own * cap + rank_row
    back = me - own_col
    back = jnp.where(back < 0, back + n_gy, back)
    to_col = back * cap + rank_col
    chosen = (iota((slots, n), 0).astype(f32) == to_row).astype(bf16)
    sel[...] = chosen
    sel_t[...] = (iota((n, slots), 1).astype(f32) == to_col).astype(bf16)
    depth = (flags[...] * tally[...]).astype(f32)
    depth_col = jnp.sum(
        jnp.where(row_i == col_i, jnp.broadcast_to(depth, (n, n)), 0.0), axis=1, keepdims=True
    )
    a = amb[...].astype(f32).reshape(bx_n, SUB, LANES)
    b = light[...].astype(f32).reshape(bx_n, SUB, LANES)
    halves = jnp.stack(join_levels(a, b), axis=1).reshape(2 * bx_n, SUB, LANES)
    rows = swap_granules(halves).reshape(n, LANES)
    fields = jnp.concatenate([rows, jnp.broadcast_to(depth_col, (n, LANES))], axis=1).astype(bf16)
    tail[...] = jnp.dot(chosen, fields, preferred_element_type=f32).astype(bf16)


def stencil_kernel(
    bx_n, by_n, t, flags, tally, fxlo, fxhi, fylo, fyhi, own_lo, own_hi, sel, tail,
    stepped, packed, blocks,
):
    levels = t.shape[0]
    width = levels * HALF
    depth = (flags[...] * tally[...]).astype(f32)
    d = depth_rows(depth, by_n)
    nx = t.shape[1]
    lane = iota((nx, LANES), 1)
    row = iota((nx, LANES), 0)
    d_lo = jnp.broadcast_to(fxlo[levels : levels + 1, :], (nx, LANES))
    d_hi = jnp.broadcast_to(fxhi[levels : levels + 1, :], (nx, LANES))
    d_at = jnp.concatenate(
        [jnp.broadcast_to(d[bx : bx + 1], (SUB, LANES)) for bx in range(bx_n)], axis=0
    )
    d_xm = jnp.where(row == 0, d_lo, pltpu.roll(d_at, 1, 0))
    d_xp = jnp.where(row == nx - 1, d_hi, pltpu.roll(d_at, nx - 1, 0))
    d_ym = jnp.where(lane == 0, 0.0, pltpu.roll(d_at, 1, 1))
    d_yp = jnp.where(lane == LANES - 1, 0.0, pltpu.roll(d_at, LANES - 1, 1))
    add_lo = fylo[SUB:, :] * (fylo[0:SUB, :] - own_lo[0:SUB, :])
    add_hi = fyhi[SUB:, :] * (fyhi[0:SUB, :] - own_hi[0:SUB, :])
    for k0 in range(0, levels, 4):
        done = []
        for k in range(k0, k0 + 4):
            kf = float(k)
            c = t[k]
            xm = jnp.where(row == 0, row_of(fxlo, k, n=nx), pltpu.roll(c, 1, 0))
            xp = jnp.where(row == nx - 1, row_of(fxhi, k, n=nx), pltpu.roll(c, nx - 1, 0))
            ym = pltpu.roll(c, 1, 1)
            yp = pltpu.roll(c, LANES - 1, 1)
            js = [k * bx_n + bx for bx in range(bx_n)]
            lo = jnp.concatenate([pltpu.roll(add_lo, (LANES - j) % LANES, 1) for j in js], axis=0)
            hi = jnp.concatenate(
                [pltpu.roll(add_hi, (LANES - 1 - j) % LANES, 1) for j in js], axis=0
            )
            total = jnp.where(d_xm > kf, xm - c, 0.0)
            total = total + jnp.where(d_xp > kf, xp - c, 0.0)
            total = total + jnp.where(lane == 0, lo, jnp.where(d_ym > kf, ym - c, 0.0))
            total = total + jnp.where(lane == LANES - 1, hi, jnp.where(d_yp > kf, yp - c, 0.0))
            s = c + jnp.where(d_at > kf, NU_COEF * total, 0.0)
            stepped[k] = s
            done.append(s.reshape(bx_n, SUB, LANES))
        halves = []
        for p in (0, 2):
            halves += list(join_levels(done[p], done[p + 1]))
        out = swap_granules(jnp.concatenate(halves, axis=0))
        for q in range(4):
            kp = k0 // 2 + q // 2
            for bx in range(bx_n):
                g = (bx * 2 + q % 2) * SUB
                blocks[g : g + SUB, kp * LANES : (kp + 1) * LANES] = out[q * bx_n + bx]
    packed[:, :width] = jnp.dot(
        sel[...], blocks[...].astype(bf16), preferred_element_type=f32
    ).astype(bf16)
    packed[:, width:] = tail[...]


def clear_kernel(n_gy, c, above, *rest):
    passed, (buf, sems) = rest[:n_gy], rest[n_gy:]
    cap = passed[0].shape[0]
    width = above.shape[1]
    me = lax.axis_index("gy")
    chunks = [lax.rem(me + i, n_gy) * cap for i in range(n_gy)]
    loads = [
        pltpu.make_async_copy(c.at[pl.ds(r, cap)], buf.at[i], sems.at[i])
        for i, r in enumerate(chunks)
    ]
    for load in loads:
        load.start()
    low = iota((cap, LANES), 1) < HALF
    spans = [slice(v * LANES, (v + 1) * LANES) for v in range(width // LANES)]
    for i, r in enumerate(chunks):
        loads[i].wait()
        a = [ATTEN_WATER + ATTEN_CHL * buf[i, :, 0, at] for at in spans]
        both = [x + pltpu.roll(x, HALF, 1) for x in a]
        carry = jnp.zeros((cap, LANES), f32)
        sums = []
        for x, y in zip(a, both):
            sums.append(carry + jnp.where(low, x, y))
            carry = carry + y
        left = [jnp.exp(-x) for x in sums]
        before = [jnp.ones((cap, LANES), f32)] + left[:-1]
        prev = [pltpu.roll(jnp.where(low, x, y), HALF, 1) for x, y in zip(left, before)]
        for at, x, y in zip(spans, prev, left):
            above[pl.ds(pl.multiple_of(r, cap), cap), at] = x
            passed[i][:, at] = (x - y).astype(bf16)


def spread_tail(arrived, rows, width):
    tail = arrived[rows, width : width + LANES].astype(f32)
    count = arrived[rows, width + LANES :].astype(f32)
    low = iota(tail.shape, 1) < HALF
    turned = pltpu.roll(tail, HALF, 1)
    return jnp.where(low, tail, turned), jnp.where(low, turned, tail), count


def chunk_loads(c, buf, sems):
    group = buf.shape[1]
    return [
        pltpu.make_async_copy(c.at[pl.ds(i * group, group)], buf.at[i], sems.at[i])
        for i in range(buf.shape[0])
    ]


def growth_kernel(arrived, above, c, weight, part, buf, sems):
    chunks, group, tracers, width = buf.shape
    for load in chunk_loads(c, buf, sems):
        load.start()
    spans = [slice(v * LANES, (v + 1) * LANES) for v in range(width // LANES)]
    half = (iota((group, LANES), 1) // HALF).astype(f32)

    def one(i, carry):
        sums, counts = list(carry[:-1]), carry[-1]
        r = pl.multiple_of(i * group, group)
        rows = pl.ds(r, group)
        _, light, count = spread_tail(arrived, rows, width)
        tops = [light * above[rows, at] for at in spans]
        temp = [jnp.exp(GROWTH_TEMP * arrived[rows, at].astype(f32)) for at in spans]
        rest = [1.0 / (x + 1.0) for x in tops]
        for v in range(len(spans)):
            g = STEP_DT * (temp[v] * (tops[v] * rest[v]))
            weight[v, rows, :] = jnp.where(half + float(2 * v) < count, g, 0.0)
        pltpu.make_async_copy(c.at[rows], buf.at[i], sems.at[i]).wait()
        for v, at in enumerate(spans):
            for s in range(group):
                sums[s % 8] = sums[s % 8] + row_of(weight, v, r + s) * buf[i, s, :, at]
        return (*sums, counts + count)

    start = (*[jnp.zeros((tracers, LANES), f32)] * 8, jnp.zeros((group, LANES), f32))
    *sums, counts = lax.fori_loop(0, chunks, one, start)
    total = functools.reduce(jnp.add, sums)
    total = total + pltpu.roll(total, HALF, 1)
    wet = jnp.broadcast_to(jnp.sum(counts, axis=0, keepdims=True), (tracers, LANES))
    line = jnp.where(iota((tracers, LANES), 1) < HALF, total, wet)
    part[...] = jnp.broadcast_to(line[None], part.shape)


def final_kernel(
    parts, arrived, weight, rates, c, out, buf, reactions, mix, mixed, fluxes, sems, out_sems
):
    chunks, group, tracers, width = buf.shape
    for load in chunk_loads(c, buf, sems):
        load.start()
    n_rows = group * tracers
    lane = iota((tracers, LANES), 1)
    steps = width // LANES
    spans = [slice(v * LANES, (v + 1) * LANES) for v in range(steps)]

    total = jnp.sum(parts[...], axis=0)
    grown = jnp.sum(jnp.where(lane < HALF, total, 0.0), axis=1, keepdims=True)
    cells = HALF * total[:, LANES - 1 :]
    change = jnp.zeros((tracers, LANES), f32)
    for s in range(tracers):
        change = change + rates[:, s : s + 1] * jnp.broadcast_to(
            grown[s : s + 1, :], (tracers, LANES)
        )
    move = (-change / jnp.maximum(cells, 1.0))[None]
    i_row = iota((n_rows, tracers), 0) % tracers == iota((n_rows, tracers), 1)
    j_col = iota((tracers, n_rows), 1) % tracers == iota((tracers, n_rows), 0)
    spread = jnp.dot(i_row.astype(f32), rates[...], preferred_element_type=f32)
    spread = jnp.dot(spread, j_col.astype(f32), preferred_element_type=f32)
    one_slot = iota((n_rows, n_rows), 0) // tracers == iota((n_rows, n_rows), 1) // tracers
    reactions[...] = jnp.where(one_slot, spread, 0.0).astype(bf16)

    half = (iota((group, LANES), 1) // HALF).astype(f32)
    low = iota((group, LANES), 1) < HALF
    low3 = iota((group, tracers, LANES), 2) < HALF

    def one(i, carry):
        r = pl.multiple_of(i * group, group)
        rows = pl.ds(r, group)
        amb, _, count = spread_tail(arrived, rows, width)
        here = [arrived[rows, at].astype(f32) for at in spans]
        below = [
            pltpu.roll(jnp.where(low, y, x), HALF, 1) for x, y in zip(here, here[1:] + here[-1:])
        ]
        bend = [jnp.tanh(x - y) for x, y in zip(here, below)]
        for v in range(steps):
            m = (amb * (1.0 + 0.5 * bend[v])).astype(bf16).astype(f32)
            mix[v] = jnp.where(half + float(2 * v + 1) < count, STEP_DT * m, 0.0)
        pltpu.make_async_copy(c.at[rows], buf.at[i], sems.at[i]).wait()
        mixed[...] = jnp.dot(
            reactions[...], buf[i].reshape(n_rows, width).astype(bf16), preferred_element_type=f32
        )

        def turned(v):
            nx = spans[min(v + 1, steps - 1)]
            return pltpu.roll(jnp.where(low3, buf[i, :, :, nx], buf[i, :, :, spans[v]]), HALF, 2)

        waiting = [turned(0), turned(1)]
        for v, at in enumerate(spans):
            if v + 2 < steps:
                waiting.append(turned(v + 2))
            spread_mix = jnp.stack([row_of(mix, v, s) for s in range(group)])
            fluxes[v] = spread_mix * (waiting.pop(0) - buf[i, :, :, at])

        def turned_flux(v):
            prev = fluxes[v - 1] if v else jnp.zeros((group, tracers, LANES), f32)
            return pltpu.roll(jnp.where(low3, fluxes[v], prev), HALF, 2)

        spare = count - half
        left = jnp.stack(
            [jnp.broadcast_to(spare[s : s + 1, :], (tracers, LANES)) for s in range(group)]
        )
        waiting = [turned_flux(0), turned_flux(1)]
        for v, at in enumerate(spans):
            if v + 2 < steps:
                waiting.append(turned_flux(v + 2))
            w = jnp.stack([row_of(weight, v, r + s) for s in range(group)])
            m = mixed[:, at].reshape(group, tracers, LANES)
            y = buf[i, :, :, at] + ((fluxes[v] - waiting.pop(0)) + w * m)
            buf[i, :, :, at] = y + jnp.where(left > float(2 * v), move, 0.0)
        pltpu.make_async_copy(buf.at[i], out.at[rows], out_sems.at[i]).start()
        return carry

    lax.fori_loop(0, chunks, one, 0)
    for i in range(chunks):
        pltpu.make_async_copy(buf.at[i], out.at[pl.ds(i * group, group)], out_sems.at[i]).wait()


def warm_kernel(bx_n, by_n, n_gy, sel_t, light, flags, tally, stepped, *rest):
    returned, (out, blocks) = rest[:n_gy], rest[n_gy:]
    levels, nx, ny = stepped.shape
    got = jnp.concatenate([r[...] for r in returned], axis=0)
    blocks[...] = jnp.dot(sel_t[...], got, preferred_element_type=f32)
    depth = (flags[...] * tally[...]).astype(f32)
    d = depth_rows(depth, by_n)
    d_at = jnp.concatenate(
        [jnp.broadcast_to(d[bx : bx + 1], (SUB, LANES)) for bx in range(bx_n)], axis=0
    )
    scale = WARMING_SCALE * light[...].astype(f32)
    for k0 in range(0, levels, 4):
        halves = []
        for q in range(4):
            kp = k0 // 2 + q // 2
            for bx in range(bx_n):
                g = (bx * 2 + q % 2) * SUB
                halves.append(blocks[g : g + SUB, kp * LANES : (kp + 1) * LANES])
        swapped = swap_granules(jnp.stack(halves))
        for p in range(2):
            lo = swapped[2 * p * bx_n : (2 * p + 1) * bx_n]
            hi = swapped[(2 * p + 1) * bx_n : (2 * p + 2) * bx_n]
            for e, took in enumerate(join_levels(lo, hi)):
                k = k0 + 2 * p + e
                out[k] = stepped[k] + jnp.where(d_at > float(k), scale * took.reshape(nx, ny), 0.0)


def vmem(n):
    return [pl.BlockSpec(memory_space=pltpu.VMEM)] * n


def shaped(shape, dtype):
    return jax.ShapeDtypeStruct(shape, dtype)


def params():
    return pltpu.CompilerParams(vmem_limit_bytes=20 << 20)


def in_hbm(x):
    return pltpu.with_memory_space_constraint(x, pltpu.HBM)


def on_device(
    thermal_anomaly,
    ambient_diffusion,
    solar_light,
    sea_tile_flags,
    flooded_layer_tally,
    tile_holder_rank,
    solute_amounts,
    reaction_rates,
):
    levels, nx, ny = thermal_anomaly.shape
    bx_n, by_n = nx // 8, ny // 8
    n_blocks = bx_n * by_n
    slots, tracers, width = solute_amounts.shape[2:]
    n_gy = lax.axis_size("gy")
    n_all = n_gy * lax.axis_size("gx")
    cap = slots // n_gy
    flags = sea_tile_flags.reshape(1, n_blocks)
    tally = flooded_layer_tally.reshape(1, n_blocks)
    holder = tile_holder_rank.reshape(1, n_blocks)
    amounts = in_hbm(solute_amounts.reshape(slots, tracers, width))

    sources = [thermal_anomaly, flags, tally, ambient_diffusion, solar_light, holder]
    xlo, xhi, ylo, yhi, *held = pl.pallas_call(
        functools.partial(edges_kernel, bx_n, by_n),
        out_shape=[shaped((levels + SUB, LANES), f32)] * 2
        + [shaped((2 * SUB, LANES), f32)] * 2
        + [shaped(x.shape, x.dtype) for x in sources],
        in_specs=[pl.BlockSpec(memory_space=pltpu.HBM)] * len(sources),
        out_specs=vmem(4 + len(sources)),
        scratch_shapes=[pltpu.SemaphoreType.DMA((len(sources),))],
        compiler_params=params(),
        name="edges",
    )(*[in_hbm(x) for x in sources])
    thermal, flags, tally, ambient, light, holder = held

    def onward(x, axis, way):
        count = lax.axis_size(axis)
        pairs = [(i, i + 1) for i in range(count - 1)]
        return lax.ppermute(x, axis, pairs if way > 0 else [(j, i) for i, j in pairs])

    fxlo = onward(xhi, "gx", 1)
    fxhi = onward(xlo, "gx", -1)
    fylo = onward(yhi, "gy", 1)
    fyhi = onward(ylo, "gy", -1)

    sel, sel_t, tail = pl.pallas_call(
        functools.partial(slots_kernel, bx_n, by_n, cap, n_gy),
        out_shape=[
            shaped((slots, n_blocks), bf16),
            shaped((n_blocks, slots), bf16),
            shaped((slots, 2 * LANES), bf16),
        ],
        in_specs=vmem(5),
        out_specs=vmem(3),
        compiler_params=params(),
        name="slots",
    )(ambient, light, flags, tally, holder)

    group = 16
    steps = slots // group
    buffers = [
        pltpu.VMEM((steps, group, tracers, width), f32),
        pltpu.SemaphoreType.DMA((steps,)),
    ]
    any_hbm = pl.BlockSpec(memory_space=pltpu.HBM)
    above, *passed = pl.pallas_call(
        functools.partial(clear_kernel, n_gy),
        out_shape=[shaped((slots, width), f32)] + [shaped((cap, width), bf16)] * n_gy,
        in_specs=[pl.BlockSpec(memory_space=pltpu.HBM)],
        out_specs=vmem(1 + n_gy),
        scratch_shapes=[
            pltpu.VMEM((n_gy, cap, tracers, width), f32),
            pltpu.SemaphoreType.DMA((n_gy,)),
        ],
        compiler_params=params(),
        name="clear",
    )(amounts)

    stepped, packed = pl.pallas_call(
        functools.partial(stencil_kernel, bx_n, by_n),
        out_shape=[shaped((levels, nx, ny), f32), shaped((slots, width + 2 * LANES), bf16)],
        in_specs=vmem(11),
        out_specs=vmem(2),
        scratch_shapes=[pltpu.VMEM((n_blocks, width), f32)],
        compiler_params=params(),
        name="stencil",
    )(thermal, flags, tally, fxlo, fxhi, fylo, fyhi, ylo, yhi, sel, tail)

    def exchange(x):
        y = lax.all_to_all(x.reshape(n_gy, cap, x.shape[1]), "gy", 0, 0, tiled=True)
        return y.reshape(x.shape)

    arrived = exchange(packed)
    returned = [passed[0]]
    for d in range(1, n_gy):
        pairs = [(i, (i + d) % n_gy) for i in range(n_gy)]
        returned.append(lax.ppermute(passed[d], "gy", pairs))

    weight, part = pl.pallas_call(
        growth_kernel,
        out_shape=[
            shaped((width // LANES, slots, LANES), f32),
            shaped((n_all, tracers, LANES), f32),
        ],
        in_specs=vmem(2) + [any_hbm],
        out_specs=vmem(2),
        scratch_shapes=buffers,
        compiler_params=params(),
        name="growth",
    )(arrived, above, amounts)

    parts = lax.all_to_all(part, ("gx", "gy"), 0, 0, tiled=True)

    out = pl.pallas_call(
        final_kernel,
        out_shape=shaped((slots, tracers, width), f32),
        in_specs=vmem(4) + [any_hbm],
        out_specs=any_hbm,
        scratch_shapes=[
            buffers[0],
            pltpu.VMEM((group * tracers, group * tracers), bf16),
            pltpu.VMEM((width // LANES, group, LANES), f32),
            pltpu.VMEM((group * tracers, width), f32),
            pltpu.VMEM((width // LANES, group, tracers, LANES), f32),
            buffers[1],
            pltpu.SemaphoreType.DMA((steps,)),
        ],
        compiler_params=params(),
        name="final",
    )(parts, arrived, weight, reaction_rates, amounts)

    thermal_final = pl.pallas_call(
        functools.partial(warm_kernel, bx_n, by_n, n_gy),
        out_shape=shaped((levels, nx, ny), f32),
        in_specs=vmem(5 + n_gy),
        out_specs=pl.BlockSpec(memory_space=pltpu.VMEM),
        scratch_shapes=[pltpu.VMEM((n_blocks, width), f32)],
        compiler_params=params(),
        name="warm",
    )(sel_t, light, flags, tally, stepped, *returned)
    return thermal_final, out.reshape(solute_amounts.shape)


def solution(mesh):
    return jax.shard_map(
        on_device,
        mesh=mesh,
        in_specs=(
            P(None, "gx", "gy"),
            P("gx", "gy"),
            P("gx", "gy"),
            P("gx", "gy", None),
            P("gx", "gy", None),
            P("gx", "gy", None, None),
            P("gx", "gy", None, None, None),
            P(),
        ),
        out_specs=(P(None, "gx", "gy"), P("gx", "gy", None, None, None)),
        check_vma=False,
    )
```

```python
import functools
import jax
import jax.numpy as jnp
from jax import lax
from jax.experimental import pallas as pl
from jax.experimental.pallas import tpu as pltpu
from jax.sharding import PartitionSpec as P

NU_COEF = 0.2
STEP_DT = 0.05
ATTEN_WATER = 0.06
ATTEN_CHL = 0.05
WARMING_SCALE = 0.5
GROWTH_TEMP = 0.063
LANES = 128
HALF = 64
SUB = 8
AHEAD = 4
DEEP = 3
BATCH = 16
WARM_BATCH = 16


f32 = jnp.float32
bf16 = jnp.bfloat16


def iota(shape, dim):
    return lax.broadcasted_iota(jnp.int32, shape, dim)


def swap_granules(x):
    row = iota(x.shape, 1)
    lane = iota(x.shape, 2)
    for step in (1, 2, 4):
        r = (row & step) != 0
        c = (lane & (step * SUB)) != 0
        w = step * SUB
        up = pltpu.roll(pltpu.roll(x, SUB - step, 1), w, 2)
        down = pltpu.roll(pltpu.roll(x, step, 1), LANES - w, 2)
        x = jnp.where(r == c, x, jnp.where(c, up, down))
    return x


def join_levels(a, b):
    low = iota(a.shape, 2) < HALF
    return (
        jnp.where(low, a, pltpu.roll(b, HALF, 2)),
        jnp.where(low, pltpu.roll(a, HALF, 2), b),
    )


def row_of(ref, *at, n=SUB):
    return ref[(*at[:-1], pl.ds(at[-1], n, stride=0), slice(None))]


def depth_rows(depth, blocks_y):
    n = depth.shape[1]
    mine = iota((SUB, n), 1) // blocks_y == iota((SUB, n), 0)
    left = jnp.where(mine, jnp.broadcast_to(depth, (SUB, n)), 0.0)
    spread = iota((n, LANES), 0) % blocks_y == iota((n, LANES), 1) // SUB
    return jnp.dot(left, spread.astype(f32), preferred_element_type=f32)


def edge_depth(depth, blocks_x, blocks_y, by):
    n = depth.shape[1]
    pick = iota((n, LANES), 0) == (iota((n, LANES), 1) % blocks_x) * blocks_y + by
    return jnp.dot(
        jnp.broadcast_to(depth, (SUB, n)), pick.astype(f32), preferred_element_type=f32
    )


def edges_kernel(bx_n, by_n, *refs):
    sources, (x1, x2, y1, y2), held, sems = refs[:6], refs[6:10], refs[10:16], refs[16]
    even_x = lax.axis_index("gx") % 2 == 0
    even_y = lax.axis_index("gy") % 2 == 0
    t, flags, tally = held[:3]
    levels, nx, _ = t.shape
    loads = [
        pltpu.make_async_copy(x, y, sems.at[i]) for i, (x, y) in enumerate(zip(sources, held))
    ]
    for load in loads:
        load.start()
    for load in loads:
        load.wait()
    depth = (flags[...] * tally[...]).astype(f32)
    d = depth_rows(depth, by_n)
    for k in range(levels):
        first, last = t[k, 0:1, :], t[k, nx - 1 : nx, :]
        x1[k : k + 1, :] = jnp.where(even_x, last, first)
        x2[k : k + 1, :] = jnp.where(even_x, first, last)
    first = jnp.broadcast_to(d[0:1], (SUB, LANES))
    last = jnp.broadcast_to(d[bx_n - 1 : bx_n], (SUB, LANES))
    x1[levels : levels + SUB, :] = jnp.where(even_x, last, first)
    x2[levels : levels + SUB, :] = jnp.where(even_x, first, last)
    lane = iota((SUB, LANES), 1)
    lo = jnp.zeros((SUB, LANES), f32)
    hi = jnp.zeros((SUB, LANES), f32)
    for k0 in range(0, levels, 4):
        places = [(k, bx) for k in range(k0, k0 + 4) for bx in range(bx_n)]
        tiles = [t[k, bx * SUB : (bx + 1) * SUB, :] for k, bx in places]
        js = [k * bx_n + bx for k, bx in places]
        los = [pltpu.roll(v, j, 1) for v, j in zip(tiles, js)]
        his = [pltpu.roll(v, (j + 1) % LANES, 1) for v, j in zip(tiles, js)]
        for j, a, b in zip(js, los, his):
            lo = jnp.where(lane == j, a, lo)
            hi = jnp.where(lane == j, b, hi)
    y1[0:SUB, :] = jnp.where(even_y, hi, lo)
    y2[0:SUB, :] = jnp.where(even_y, lo, hi)
    k_lane = (lane // bx_n).astype(f32)
    in_lo = (k_lane < edge_depth(depth, bx_n, by_n, 0)).astype(f32)
    in_hi = (k_lane < edge_depth(depth, bx_n, by_n, by_n - 1)).astype(f32)
    y1[SUB:, :] = jnp.where(even_y, in_hi, in_lo)
    y2[SUB:, :] = jnp.where(even_y, in_lo, in_hi)


def ranks(holder):
    n = holder.shape[1]
    row_i = iota((n, n), 0)
    col_i = iota((n, n), 1)
    own = holder[...].astype(f32)
    own_row = jnp.broadcast_to(own, (n, n))
    own_col = jnp.sum(jnp.where(row_i == col_i, own_row, 0.0), axis=1, keepdims=True)
    same = own_row == own_col
    rank_row = jnp.sum(jnp.where(same & (row_i < col_i), 1.0, 0.0), axis=0, keepdims=True)
    rank_col = jnp.sum(jnp.where(same & (col_i < row_i), 1.0, 0.0), axis=1, keepdims=True)
    return own, rank_row, own_col, rank_col


def slots_kernel(bx_n, by_n, cap, amb, light, flags, tally, holder, sel, tail):
    n = bx_n * by_n
    slots = sel.shape[0]
    _, rank_row, _, _ = ranks(holder)
    turn = jnp.bitwise_xor(holder[...], lax.axis_index("gy")).astype(f32)
    chosen = (iota((slots, n), 0).astype(f32) == turn * cap + rank_row).astype(bf16)
    sel[...] = chosen
    row_i = iota((n, n), 0)
    col_i = iota((n, n), 1)
    depth = (flags[...] * tally[...]).astype(f32)
    depth_col = jnp.sum(
        jnp.where(row_i == col_i, jnp.broadcast_to(depth, (n, n)), 0.0), axis=1, keepdims=True
    )
    a = amb[...].astype(f32).reshape(bx_n, SUB, LANES)
    b = light[...].astype(f32).reshape(bx_n, SUB, LANES)
    halves = jnp.stack(join_levels(a, b), axis=1).reshape(2 * bx_n, SUB, LANES)
    rows = swap_granules(halves).reshape(n, LANES)
    fields = jnp.concatenate([rows, jnp.broadcast_to(depth_col, (n, LANES))], axis=1).astype(bf16)
    tail[...] = jnp.dot(chosen, fields, preferred_element_type=f32).astype(bf16)


def stencil_kernel(
    bx_n, by_n, t, flags, tally, x1, x2, y1, y2, own_1, own_2, sel, tail, stepped_hbm, *rest
):
    packed, (blocks, fxlo, fxhi, stepped, sems) = rest[:-5], rest[-5:]
    sends = []
    even_x = lax.axis_index("gx") % 2 == 0
    even_y = lax.axis_index("gy") % 2 == 0
    fxlo[...] = jnp.where(even_x, x2[...], x1[...])
    fxhi[...] = jnp.where(even_x, x1[...], x2[...])
    add_1 = y1[SUB:, :] * (y1[0:SUB, :] - own_1[0:SUB, :])
    add_2 = y2[SUB:, :] * (y2[0:SUB, :] - own_2[0:SUB, :])
    add_lo = jnp.where(even_y, add_2, add_1)
    add_hi = jnp.where(even_y, add_1, add_2)
    levels = t.shape[0]
    width = levels * HALF
    depth = (flags[...] * tally[...]).astype(f32)
    d = depth_rows(depth, by_n)
    nx = t.shape[1]
    some = BATCH
    lane = iota((nx, LANES), 1)
    row = iota((nx, LANES), 0)
    d_lo = jnp.broadcast_to(fxlo[levels : levels + 1, :], (nx, LANES))
    d_hi = jnp.broadcast_to(fxhi[levels : levels + 1, :], (nx, LANES))
    d_at = jnp.concatenate(
        [jnp.broadcast_to(d[bx : bx + 1], (SUB, LANES)) for bx in range(bx_n)], axis=0
    )
    d_xm = jnp.where(row == 0, d_lo, pltpu.roll(d_at, 1, 0))[None]
    d_xp = jnp.where(row == nx - 1, d_hi, pltpu.roll(d_at, nx - 1, 0))[None]
    d_ym = jnp.where(lane == 0, 0.0, pltpu.roll(d_at, 1, 1))[None]
    d_yp = jnp.where(lane == LANES - 1, 0.0, pltpu.roll(d_at, LANES - 1, 1))[None]
    d_at = d_at[None]
    row = iota((some, nx, LANES), 1)
    lane = iota((some, nx, LANES), 2)
    for k0 in range(0, levels, some):
        ks = range(k0, k0 + some)
        kf = (k0 + iota((some, 1, 1), 0)).astype(f32)
        c = t[k0 : k0 + some]
        xm = pltpu.roll(c, 1, 1)
        xp = pltpu.roll(c, nx - 1, 1)
        ym = pltpu.roll(c, 1, 2)
        yp = pltpu.roll(c, LANES - 1, 2)
        edges = []
        for add, to in ((add_lo, 0), (add_hi, LANES - 1)):
            js = range(k0 * bx_n, (k0 + some) * bx_n)
            rolled = [pltpu.roll(add, (to - j) % LANES, 1) for j in js]
            edges.append(jnp.concatenate(rolled, axis=0).reshape(some, nx, LANES))
        xm = jnp.where(row == 0, jnp.stack([row_of(fxlo, k, n=nx) for k in ks]), xm)
        xp = jnp.where(row == nx - 1, jnp.stack([row_of(fxhi, k, n=nx) for k in ks]), xp)
        total = jnp.where(d_xm > kf, xm - c, 0.0)
        total = total + jnp.where(d_xp > kf, xp - c, 0.0)
        total = total + jnp.where(lane == 0, edges[0], jnp.where(d_ym > kf, ym - c, 0.0))
        total = total + jnp.where(lane == LANES - 1, edges[1], jnp.where(d_yp > kf, yp - c, 0.0))
        s = c + jnp.where(d_at > kf, NU_COEF * total, 0.0)
        stepped[k0 : k0 + some] = s
        rows = pl.ds(k0, some)
        sends.append(
            pltpu.make_async_copy(stepped.at[rows], stepped_hbm.at[rows], sems.at[len(sends)])
        )
        sends[-1].start()
        done = s.reshape(some, bx_n, SUB, LANES)
        halves = []
        for p in range(0, some, 2):
            halves += list(join_levels(done[p], done[p + 1]))
        out = swap_granules(jnp.concatenate(halves, axis=0))
        for q in range(some):
            kp = k0 // 2 + q // 2
            for bx in range(bx_n):
                g = (bx * 2 + q % 2) * SUB
                blocks[g : g + SUB, kp * LANES : (kp + 1) * LANES] = out[q * bx_n + bx]
    chosen = jnp.dot(sel[...], blocks[...].astype(bf16), preferred_element_type=f32).astype(bf16)
    cap = packed[0].shape[0]
    for i, chunk in enumerate(packed):
        chunk[:, :width] = chosen[i * cap : (i + 1) * cap]
        chunk[:, width:] = tail[i * cap : (i + 1) * cap]
    for send in sends:
        send.wait()


def clear_kernel(n_gy, c, above, buf, *rest):
    sent, (passed, sems, out_sems) = rest[:n_gy], rest[n_gy:]
    cap = passed.shape[1]
    width = above.shape[1]
    me = lax.axis_index("gy")
    chunks = [jnp.bitwise_xor(me, i) * cap for i in range(n_gy)]
    loads = [
        pltpu.make_async_copy(c.at[pl.ds(r, cap)], buf.at[i], sems.at[i])
        for i, r in enumerate(chunks)
    ]
    sends = [pltpu.make_async_copy(passed.at[i], sent[i], out_sems.at[i]) for i in range(n_gy)]
    for load in loads:
        load.start()
    low = iota((cap, LANES), 1) < HALF
    spans = [slice(v * LANES, (v + 1) * LANES) for v in range(width // LANES)]
    for i in range(n_gy):
        loads[i].wait()
        a = [ATTEN_WATER + ATTEN_CHL * buf[i, :, 0, at] for at in spans]
        both = [x + pltpu.roll(x, HALF, 1) for x in a]
        carry = jnp.zeros((cap, LANES), f32)
        sums = []
        for x, y in zip(a, both):
            sums.append(carry + jnp.where(low, x, y))
            carry = carry + y
        left = [jnp.exp(-x) for x in sums]
        before = [jnp.ones((cap, LANES), f32)] + left[:-1]
        prev = [pltpu.roll(jnp.where(low, x, y), HALF, 1) for x, y in zip(left, before)]
        for at, x, y in zip(spans, prev, left):
            above[i * cap : (i + 1) * cap, at] = x
            passed[i, :, at] = (x - y).astype(bf16)
        sends[i].start()
    for send in sends:
        send.wait()


def spread_tail(arrived, rows, width):
    tail = arrived[rows, width : width + LANES].astype(f32)
    count = arrived[rows, width + LANES :].astype(f32)
    low = iota(tail.shape, 1) < HALF
    turned = pltpu.roll(tail, HALF, 1)
    return jnp.where(low, tail, turned), jnp.where(low, turned, tail), count


def growth_kernel(n_gy, above, c, *rest):
    came, (arrived, weight, part) = rest[:n_gy], rest[n_gy:]
    chunks, group, tracers, width = c.shape
    for i, chunk in enumerate(came):
        arrived[i * group : (i + 1) * group, :] = chunk[...]
    spans = [slice(v * LANES, (v + 1) * LANES) for v in range(width // LANES)]
    half = (iota((group, LANES), 1) // HALF).astype(f32)

    def weigh(i):
        rows = pl.ds(pl.multiple_of(i * group, group), group)
        _, light, count = spread_tail(arrived, rows, width)
        tops = [light * above[rows, at] for at in spans]
        temp = [jnp.exp(GROWTH_TEMP * arrived[rows, at].astype(f32)) for at in spans]
        rest = [1.0 / (x + 1.0) for x in tops]
        for v in range(len(spans)):
            g = STEP_DT * (temp[v] * (tops[v] * rest[v]))
            weight[v, rows, :] = jnp.where(half + float(2 * v) < count, g, 0.0)
        return count

    def gather(i, sums):
        r = pl.multiple_of(i * group, group)
        sums = list(sums)
        for v, at in enumerate(spans):
            for s in range(group):
                sums[s % 8] = sums[s % 8] + row_of(weight, v, r + s) * c[i, s, :, at]
        return sums

    def one(i, carry):
        sums = gather(i - 1, carry[:-1])
        return (*sums, carry[-1] + weigh(i))

    start = (*[jnp.zeros((tracers, LANES), f32)] * 8, weigh(0))
    *sums, counts = lax.fori_loop(1, chunks, one, start)
    sums = gather(chunks - 1, sums)
    total = functools.reduce(jnp.add, sums)
    total = total + pltpu.roll(total, HALF, 1)
    wet = jnp.broadcast_to(jnp.sum(counts, axis=0, keepdims=True), (tracers, LANES))
    line = jnp.where(iota((tracers, LANES), 1) < HALF, total, wet)
    part[...] = jnp.broadcast_to(line[None], part.shape)


def mixing_kernel(arrived, mix):
    steps, slots, _ = mix.shape
    width = steps * LANES
    group = 16
    half = (iota((group, LANES), 1) // HALF).astype(f32)
    low = iota((group, LANES), 1) < HALF
    spans = [slice(v * LANES, (v + 1) * LANES) for v in range(steps)]

    def one(i, carry):
        rows = pl.ds(pl.multiple_of(i * group, group), group)
        amb, _, count = spread_tail(arrived, rows, width)
        here = [arrived[rows, at].astype(f32) for at in spans]
        below = [
            pltpu.roll(jnp.where(low, y, x), HALF, 1) for x, y in zip(here, here[1:] + here[-1:])
        ]
        bend = [jnp.tanh(x - y) for x, y in zip(here, below)]
        for v in range(steps):
            m = (amb * (1.0 + 0.5 * bend[v])).astype(bf16).astype(f32)
            mix[v, rows, :] = jnp.where(half + float(2 * v + 1) < count, STEP_DT * m, 0.0)
        return carry

    lax.fori_loop(0, slots // group, one, 0)


def final_kernel(
    cap, parts, arrived, weight, mix, rates_hbm, c, out, done, buf, rates, reactions, mix_up, mixed,
    sems, out_sems, rates_sem,
):
    chunks, group, tracers, width = buf.shape
    me = lax.axis_index("gy")
    rates_load = pltpu.make_async_copy(rates_hbm, rates, rates_sem)
    rates_load.start()

    def load(i):
        at = i * group
        r = jnp.bitwise_xor(me, at // cap) * cap + at % cap
        return c.at[pl.ds(r, group)], buf.at[i], out.at[pl.ds(r, group)]

    def start(i):
        source, kept, _ = load(i)
        pltpu.make_async_copy(source, kept, sems.at[i]).start()

    for i in range(AHEAD):
        start(i)
    rates_load.wait()
    n_rows = group * tracers
    lane = iota((tracers, LANES), 1)
    steps = width // LANES
    spans = [slice(v * LANES, (v + 1) * LANES) for v in range(steps)]

    total = jnp.sum(parts[...], axis=0)
    grown = jnp.sum(jnp.where(lane < HALF, total, 0.0), axis=1, keepdims=True)
    cells = HALF * total[:, LANES - 1 :]
    change = jnp.zeros((tracers, LANES), f32)
    for s in range(tracers):
        change = change + rates[:, s : s + 1] * jnp.broadcast_to(
            grown[s : s + 1, :], (tracers, LANES)
        )
    move = (-change / jnp.maximum(cells, 1.0))[None]
    i_row = iota((n_rows, tracers), 0) % tracers == iota((n_rows, tracers), 1)
    j_col = iota((tracers, n_rows), 1) % tracers == iota((tracers, n_rows), 0)
    spread = jnp.dot(i_row.astype(f32), rates[...], preferred_element_type=f32)
    spread = jnp.dot(spread, j_col.astype(f32), preferred_element_type=f32)
    one_slot = iota((n_rows, n_rows), 0) // tracers == iota((n_rows, n_rows), 1) // tracers
    reactions[...] = jnp.where(one_slot, spread, 0.0).astype(bf16)

    half = (iota((group, LANES), 1) // HALF).astype(f32)
    low = iota((group, LANES), 1) < HALF
    low3 = iota((4, tracers, LANES), 2) < HALF

    def one(i, carry):
        r = pl.multiple_of(i * group, group)
        rows = pl.ds(r, group)

        @pl.when(i + AHEAD < chunks)
        def _():
            start(i + AHEAD)

        source, kept_at, goes = load(i)
        pltpu.make_async_copy(source, kept_at, sems.at[i]).wait()
        count = arrived[rows, width + LANES :].astype(f32)
        kept = [mix[v, rows, :] for v in range(steps)]
        zero = jnp.zeros_like(kept[0])
        for v, (x, y) in enumerate(zip(kept, [zero] + kept[:-1])):
            mix_up[v] = pltpu.roll(jnp.where(low, x, y), HALF, 1)
        mixed[...] = jnp.dot(
            reactions[...], buf[i].reshape(n_rows, width).astype(bf16), preferred_element_type=f32
        )

        spare = count - half
        for s0 in range(0, group, 4):
            some = range(s0, s0 + 4)
            left = jnp.stack(
                [jnp.broadcast_to(spare[s : s + 1, :], (tracers, LANES)) for s in some]
            )
            at_v = lambda v: buf[i, s0 : s0 + 4, :, spans[min(v, steps - 1)]]
            stacked = lambda ref, v, r0: jnp.stack([row_of(ref, v, r0 + s) for s in some])
            turn = lambda x, y: pltpu.roll(jnp.where(low3, y, x), HALF, 2)
            xs = [at_v(v) for v in range(DEEP + 1)]
            turns = [turn(xs[v], xs[v + 1]) for v in range(DEEP)]
            before = pltpu.roll(xs[0], HALF, 2)
            for v, at in enumerate(spans):
                xs.append(at_v(v + DEEP + 1))
                turns.append(turn(xs[DEEP], xs[DEEP + 1]))
                x, z = xs.pop(0), turns.pop(0)
                m = mixed[s0 * tracers : (s0 + 4) * tracers, at].reshape(4, tracers, LANES)
                flux = stacked(mix, v, r) * (z - x) - stacked(mix_up, v, 0) * (x - before)
                y = x + (flux + stacked(weight, v, r) * m)
                buf[i, s0 : s0 + 4, :, at] = y + jnp.where(left > float(2 * v), move, 0.0)
                before = z
        pltpu.make_async_copy(kept_at, goes, out_sems.at[i]).start()
        return carry

    lax.fori_loop(0, chunks, one, 0)
    done[...] = move[0]
    for i in range(chunks):
        _, kept_at, goes = load(i)
        pltpu.make_async_copy(kept_at, goes, out_sems.at[i]).wait()


def warm_kernel(bx_n, by_n, n_gy, holder, light, flags, tally, stepped_hbm, _, *rest):
    returned, (out, blocks, stepped, sem) = rest[:n_gy], rest[n_gy:]
    fetch = pltpu.make_async_copy(stepped_hbm, stepped, sem)
    fetch.start()
    levels, nx, ny = stepped.shape
    cap = returned[0].shape[0]
    n = bx_n * by_n
    _, _, own_col, rank_col = ranks(holder)
    turn = jnp.bitwise_xor(own_col.astype(jnp.int32), lax.axis_index("gy")).astype(f32)
    to_col = turn * cap + rank_col
    sel_t = (iota((n, n_gy * cap), 1).astype(f32) == to_col).astype(bf16)
    got = jnp.concatenate([r[...] for r in returned], axis=0)
    blocks[...] = jnp.dot(sel_t, got, preferred_element_type=f32)
    depth = (flags[...] * tally[...]).astype(f32)
    d = depth_rows(depth, by_n)
    d_at = jnp.concatenate(
        [jnp.broadcast_to(d[bx : bx + 1], (SUB, LANES)) for bx in range(bx_n)], axis=0
    )
    scale = WARMING_SCALE * light[...].astype(f32)
    fetch.wait()
    for k0 in range(0, levels, WARM_BATCH):
        halves = []
        for q in range(WARM_BATCH):
            kp = k0 // 2 + q // 2
            for bx in range(bx_n):
                g = (bx * 2 + q % 2) * SUB
                halves.append(blocks[g : g + SUB, kp * LANES : (kp + 1) * LANES])
        swapped = swap_granules(jnp.stack(halves))
        for p in range(WARM_BATCH // 2):
            lo = swapped[2 * p * bx_n : (2 * p + 1) * bx_n]
            hi = swapped[(2 * p + 1) * bx_n : (2 * p + 2) * bx_n]
            for e, took in enumerate(join_levels(lo, hi)):
                k = k0 + 2 * p + e
                out[k] = stepped[k] + jnp.where(d_at > float(k), scale * took.reshape(nx, ny), 0.0)


def vmem(n):
    return [pl.BlockSpec(memory_space=pltpu.VMEM)] * n


def shaped(shape, dtype):
    return jax.ShapeDtypeStruct(shape, dtype)


def params():
    return pltpu.CompilerParams(vmem_limit_bytes=20 << 20)


def in_hbm(x):
    return pltpu.with_memory_space_constraint(x, pltpu.HBM)


def on_device(
    thermal_anomaly,
    ambient_diffusion,
    solar_light,
    sea_tile_flags,
    flooded_layer_tally,
    tile_holder_rank,
    solute_amounts,
    reaction_rates,
):
    levels, nx, ny = thermal_anomaly.shape
    bx_n, by_n = nx // 8, ny // 8
    n_blocks = bx_n * by_n
    slots, tracers, width = solute_amounts.shape[2:]
    n_gy = lax.axis_size("gy")
    n_all = n_gy * lax.axis_size("gx")
    cap = slots // n_gy
    flags = sea_tile_flags.reshape(1, n_blocks)
    tally = flooded_layer_tally.reshape(1, n_blocks)
    holder = tile_holder_rank.reshape(1, n_blocks)
    amounts = in_hbm(solute_amounts.reshape(slots, tracers, width))

    sources = [thermal_anomaly, flags, tally, ambient_diffusion, solar_light, holder]
    x1, x2, y1, y2, *held = pl.pallas_call(
        functools.partial(edges_kernel, bx_n, by_n),
        out_shape=[shaped((levels + SUB, LANES), f32)] * 2
        + [shaped((2 * SUB, LANES), f32)] * 2
        + [pltpu.VMEM(x.shape, x.dtype) for x in sources],
        in_specs=[pl.BlockSpec(memory_space=pltpu.HBM)] * len(sources),
        out_specs=vmem(4 + len(sources)),
        scratch_shapes=[pltpu.SemaphoreType.DMA((len(sources),))],
        compiler_params=params(),
        name="edges",
    )(*[in_hbm(x) for x in sources])
    thermal, flags, tally, ambient, light, holder = held

    def traded(x, axis, first):
        count = lax.axis_size(axis)
        pairs = [(i, i + 1) for i in range(first, count - 1, 2)]
        return lax.ppermute(x, axis, pairs + [(j, i) for i, j in pairs])

    far_y2 = traded(y2, "gy", 1)
    far_x2 = traded(x2, "gx", 1)
    far_y1 = traded(y1, "gy", 0)
    far_x1 = traded(x1, "gx", 0)

    sel, tail = pl.pallas_call(
        functools.partial(slots_kernel, bx_n, by_n, cap),
        out_shape=[
            shaped((slots, n_blocks), bf16),
            shaped((slots, 2 * LANES), bf16),
        ],
        in_specs=vmem(5),
        out_specs=vmem(2),
        compiler_params=params(),
        name="slots",
    )(ambient, light, flags, tally, holder)

    group = min(16, cap)
    steps = slots // group
    buffers = [
        pltpu.VMEM((steps, group, tracers, width), f32),
        pltpu.SemaphoreType.DMA((steps,)),
    ]
    any_hbm = pl.BlockSpec(memory_space=pltpu.HBM)
    above, held_amounts, *passed = pl.pallas_call(
        functools.partial(clear_kernel, n_gy),
        out_shape=[
            pltpu.VMEM((slots, width), f32),
            pltpu.VMEM((n_gy, cap, tracers, width), f32),
        ]
        + [pltpu.HBM((cap, width), bf16)] * n_gy,
        in_specs=[any_hbm],
        out_specs=vmem(2) + [any_hbm] * n_gy,
        scratch_shapes=[
            pltpu.VMEM((n_gy, cap, width), bf16),
            pltpu.SemaphoreType.DMA((n_gy,)),
            pltpu.SemaphoreType.DMA((n_gy,)),
        ],
        compiler_params=params(),
        name="clear",
    )(amounts)

    stepped, *packed = pl.pallas_call(
        functools.partial(stencil_kernel, bx_n, by_n),
        out_shape=[pltpu.HBM((levels, nx, ny), f32)]
        + [shaped((cap, width + 2 * LANES), bf16)] * n_gy,
        in_specs=vmem(11),
        out_specs=[any_hbm] + vmem(n_gy),
        scratch_shapes=[pltpu.VMEM((n_blocks, width), f32)]
        + [pltpu.VMEM((levels + SUB, LANES), f32)] * 2
        + [pltpu.VMEM((levels, nx, ny), f32), pltpu.SemaphoreType.DMA((levels // BATCH,))],
        compiler_params=params(),
        name="stencil",
    )(thermal, flags, tally, far_x1, far_x2, far_y1, far_y2, y1, y2, sel, tail)

    def swapped(x, d):
        return lax.ppermute(x, "gy", [(i, i ^ d) for i in range(n_gy)])

    came = [packed[0]]
    for d in range(1, n_gy):
        came.append(swapped(packed[d], d))

    arrived, weight, part = pl.pallas_call(
        functools.partial(growth_kernel, n_gy),
        out_shape=[
            shaped((slots, width + 2 * LANES), bf16),
            shaped((width // LANES, slots, LANES), f32),
            shaped((n_all, tracers, LANES), f32),
        ],
        in_specs=vmem(2 + n_gy),
        out_specs=vmem(3),
        compiler_params=params(),
        name="growth",
    )(
        pltpu.with_memory_space_constraint(above, pltpu.VMEM),
        pltpu.with_memory_space_constraint(held_amounts, pltpu.VMEM),
        *came,
    )

    parts = lax.all_to_all(part, ("gx", "gy"), 0, 0, tiled=True)
    returned = [passed[0]]
    for d in range(1, n_gy):
        returned.append(swapped(passed[d], d))

    mix = pl.pallas_call(
        mixing_kernel,
        out_shape=shaped((width // LANES, slots, LANES), f32),
        in_specs=vmem(1),
        out_specs=pl.BlockSpec(memory_space=pltpu.VMEM),
        compiler_params=params(),
        name="mixing",
    )(arrived)
    by_lane = pltpu.VMEM((width // LANES, group, LANES), f32)
    out, done = pl.pallas_call(
        functools.partial(final_kernel, cap),
        out_shape=[shaped((slots, tracers, width), f32), shaped((tracers, LANES), f32)],
        in_specs=vmem(4) + [any_hbm] * 2,
        out_specs=[any_hbm] + vmem(1),
        scratch_shapes=[
            buffers[0],
            pltpu.VMEM((tracers, tracers), f32),
            pltpu.VMEM((group * tracers, group * tracers), bf16),
            by_lane,
            pltpu.VMEM((group * tracers, width), f32),
            buffers[1],
            buffers[1],
            pltpu.SemaphoreType.DMA,
        ],
        compiler_params=params(),
        name="final",
    )(parts, arrived, weight, mix, in_hbm(reaction_rates), amounts)

    thermal_final = pl.pallas_call(
        functools.partial(warm_kernel, bx_n, by_n, n_gy),
        out_shape=shaped((levels, nx, ny), f32),
        in_specs=vmem(4) + [any_hbm] + vmem(1 + n_gy),
        out_specs=pl.BlockSpec(memory_space=pltpu.VMEM),
        scratch_shapes=[
            pltpu.VMEM((n_blocks, width), f32),
            pltpu.VMEM((levels, nx, ny), f32),
            pltpu.SemaphoreType.DMA,
        ],
        compiler_params=params(),
        name="warm",
    )(holder, light, flags, tally, in_hbm(stepped), done, *returned)
    return thermal_final, out.reshape(solute_amounts.shape)


def solution(mesh):
    return jax.shard_map(
        on_device,
        mesh=mesh,
        in_specs=(
            P(None, "gx", "gy"),
            P("gx", "gy"),
            P("gx", "gy"),
            P("gx", "gy", None),
            P("gx", "gy", None),
            P("gx", "gy", None, None),
            P("gx", "gy", None, None, None),
            P(),
        ),
        out_specs=(P(None, "gx", "gy"), P("gx", "gy", None, None, None)),
        check_vma=False,
    )
```

```python
import functools
import jax
import jax.numpy as jnp
from jax import lax
from jax.experimental import pallas as pl
from jax.experimental.pallas import tpu as pltpu
from jax.sharding import PartitionSpec as P

NU_COEF = 0.2
STEP_DT = 0.05
ATTEN_WATER = 0.06
ATTEN_CHL = 0.05
WARMING_SCALE = 0.5
GROWTH_TEMP = 0.063
DRY = 2.0**100
WET = 2.0**50
LANES = 128
HALF = 64
SUB = 8
AHEAD = 4
DEEP = 3
BATCH = 16
WARM_BATCH = 16


f32 = jnp.float32
bf16 = jnp.bfloat16


def iota(shape, dim):
    return lax.broadcasted_iota(jnp.int32, shape, dim)


def swap_granules(x):
    row = iota(x.shape, 1)
    lane = iota(x.shape, 2)
    for step in (1, 2, 4):
        r = (row & step) != 0
        c = (lane & (step * SUB)) != 0
        w = step * SUB
        up = pltpu.roll(pltpu.roll(x, SUB - step, 1), w, 2)
        down = pltpu.roll(pltpu.roll(x, step, 1), LANES - w, 2)
        x = jnp.where(r == c, x, jnp.where(c, up, down))
    return x


def join_levels(a, b):
    low = iota(a.shape, 2) < HALF
    return (
        jnp.where(low, a, pltpu.roll(b, HALF, 2)),
        jnp.where(low, pltpu.roll(a, HALF, 2), b),
    )


def row_of(ref, *at, n=SUB):
    return ref[(*at[:-1], pl.ds(at[-1], n, stride=0), slice(None))]


def depth_rows(depth, blocks_y):
    n = depth.shape[1]
    mine = iota((SUB, n), 1) // blocks_y == iota((SUB, n), 0)
    left = jnp.where(mine, jnp.broadcast_to(depth, (SUB, n)), 0.0)
    spread = iota((n, LANES), 0) % blocks_y == iota((n, LANES), 1) // SUB
    return jnp.dot(left, spread.astype(f32), preferred_element_type=f32)


def edge_depth(depth, blocks_x, blocks_y, by):
    n = depth.shape[1]
    pick = iota((n, LANES), 0) == (iota((n, LANES), 1) % blocks_x) * blocks_y + by
    return jnp.dot(
        jnp.broadcast_to(depth, (SUB, n)), pick.astype(f32), preferred_element_type=f32
    )


def edges_kernel(bx_n, by_n, *refs):
    sources, (x1, x2, y1, y2), held, sems = refs[:6], refs[6:10], refs[10:16], refs[16]
    even_x = lax.axis_index("gx") % 2 == 0
    even_y = lax.axis_index("gy") % 2 == 0
    t, flags, tally = held[:3]
    levels, nx, _ = t.shape
    loads = [
        pltpu.make_async_copy(x, y, sems.at[i]) for i, (x, y) in enumerate(zip(sources, held))
    ]
    for load in loads:
        load.start()
    for load in loads:
        load.wait()
    depth = (flags[...] * tally[...]).astype(f32)
    d = depth_rows(depth, by_n)
    for k in range(levels):
        first, last = t[k, 0:1, :], t[k, nx - 1 : nx, :]
        x1[k : k + 1, :] = jnp.where(even_x, last, first)
        x2[k : k + 1, :] = jnp.where(even_x, first, last)
    first = jnp.broadcast_to(d[0:1], (SUB, LANES))
    last = jnp.broadcast_to(d[bx_n - 1 : bx_n], (SUB, LANES))
    x1[levels : levels + SUB, :] = jnp.where(even_x, last, first)
    x2[levels : levels + SUB, :] = jnp.where(even_x, first, last)
    lane = iota((SUB, LANES), 1)
    lo = jnp.zeros((SUB, LANES), f32)
    hi = jnp.zeros((SUB, LANES), f32)
    for k0 in range(0, levels, 4):
        places = [(k, bx) for k in range(k0, k0 + 4) for bx in range(bx_n)]
        tiles = [t[k, bx * SUB : (bx + 1) * SUB, :] for k, bx in places]
        js = [k * bx_n + bx for k, bx in places]
        los = [pltpu.roll(v, j, 1) for v, j in zip(tiles, js)]
        his = [pltpu.roll(v, (j + 1) % LANES, 1) for v, j in zip(tiles, js)]
        for j, a, b in zip(js, los, his):
            lo = jnp.where(lane == j, a, lo)
            hi = jnp.where(lane == j, b, hi)
    y1[0:SUB, :] = jnp.where(even_y, hi, lo)
    y2[0:SUB, :] = jnp.where(even_y, lo, hi)
    k_lane = (lane // bx_n).astype(f32)
    in_lo = (k_lane < edge_depth(depth, bx_n, by_n, 0)).astype(f32)
    in_hi = (k_lane < edge_depth(depth, bx_n, by_n, by_n - 1)).astype(f32)
    y1[SUB:, :] = jnp.where(even_y, in_hi, in_lo)
    y2[SUB:, :] = jnp.where(even_y, in_lo, in_hi)


def ranks(holder):
    n = holder.shape[1]
    row_i = iota((n, n), 0)
    col_i = iota((n, n), 1)
    own = holder[...].astype(f32)
    own_row = jnp.broadcast_to(own, (n, n))
    own_col = jnp.sum(jnp.where(row_i == col_i, own_row, 0.0), axis=1, keepdims=True)
    same = own_row == own_col
    rank_row = jnp.sum(jnp.where(same & (row_i < col_i), 1.0, 0.0), axis=0, keepdims=True)
    rank_col = jnp.sum(jnp.where(same & (col_i < row_i), 1.0, 0.0), axis=1, keepdims=True)
    return own, rank_row, own_col, rank_col


def slots_kernel(bx_n, by_n, cap, amb, light, holder, sel, tail):
    n = bx_n * by_n
    slots = sel.shape[0]
    _, rank_row, _, _ = ranks(holder)
    turn = jnp.bitwise_xor(holder[...], lax.axis_index("gy")).astype(f32)
    chosen = (iota((slots, n), 0).astype(f32) == turn * cap + rank_row).astype(bf16)
    sel[...] = chosen
    a = amb[...].astype(f32).reshape(bx_n, SUB, LANES)
    b = light[...].astype(f32).reshape(bx_n, SUB, LANES)
    halves = jnp.stack(join_levels(a, b), axis=1).reshape(2 * bx_n, SUB, LANES)
    rows = swap_granules(halves).reshape(n, LANES).astype(bf16)
    tail[...] = jnp.dot(chosen, rows, preferred_element_type=f32).astype(bf16)


def stencil_kernel(
    bx_n, by_n, t, flags, tally, x1, x2, y1, y2, own_1, own_2, sel, tail, stepped_hbm, *rest
):
    packed, (blocks, fxlo, fxhi, stepped, sems) = rest[:-5], rest[-5:]
    sends = []
    even_x = lax.axis_index("gx") % 2 == 0
    even_y = lax.axis_index("gy") % 2 == 0
    fxlo[...] = jnp.where(even_x, x2[...], x1[...])
    fxhi[...] = jnp.where(even_x, x1[...], x2[...])
    add_1 = y1[SUB:, :] * (y1[0:SUB, :] - own_1[0:SUB, :])
    add_2 = y2[SUB:, :] * (y2[0:SUB, :] - own_2[0:SUB, :])
    add_lo = jnp.where(even_y, add_2, add_1)
    add_hi = jnp.where(even_y, add_1, add_2)
    levels = t.shape[0]
    width = levels * HALF
    depth = (flags[...] * tally[...]).astype(f32)
    d = depth_rows(depth, by_n)
    nx = t.shape[1]
    some = BATCH
    lane = iota((nx, LANES), 1)
    row = iota((nx, LANES), 0)
    d_lo = jnp.broadcast_to(fxlo[levels : levels + 1, :], (nx, LANES))
    d_hi = jnp.broadcast_to(fxhi[levels : levels + 1, :], (nx, LANES))
    d_at = jnp.concatenate(
        [jnp.broadcast_to(d[bx : bx + 1], (SUB, LANES)) for bx in range(bx_n)], axis=0
    )
    d_xm = jnp.where(row == 0, d_lo, pltpu.roll(d_at, 1, 0))[None]
    d_xp = jnp.where(row == nx - 1, d_hi, pltpu.roll(d_at, nx - 1, 0))[None]
    d_ym = jnp.where(lane == 0, 0.0, pltpu.roll(d_at, 1, 1))[None]
    d_yp = jnp.where(lane == LANES - 1, 0.0, pltpu.roll(d_at, LANES - 1, 1))[None]
    d_at = d_at[None]
    row = iota((some, nx, LANES), 1)
    lane = iota((some, nx, LANES), 2)
    for k0 in range(0, levels, some):
        ks = range(k0, k0 + some)
        kf = (k0 + iota((some, 1, 1), 0)).astype(f32)
        c = t[k0 : k0 + some]
        xm = pltpu.roll(c, 1, 1)
        xp = pltpu.roll(c, nx - 1, 1)
        ym = pltpu.roll(c, 1, 2)
        yp = pltpu.roll(c, LANES - 1, 2)
        edges = []
        for add, to in ((add_lo, 0), (add_hi, LANES - 1)):
            js = range(k0 * bx_n, (k0 + some) * bx_n)
            rolled = [pltpu.roll(add, (to - j) % LANES, 1) for j in js]
            edges.append(jnp.concatenate(rolled, axis=0).reshape(some, nx, LANES))
        xm = jnp.where(row == 0, jnp.stack([row_of(fxlo, k, n=nx) for k in ks]), xm)
        xp = jnp.where(row == nx - 1, jnp.stack([row_of(fxhi, k, n=nx) for k in ks]), xp)
        total = jnp.where(d_xm > kf, xm - c, 0.0)
        total = total + jnp.where(d_xp > kf, xp - c, 0.0)
        total = total + jnp.where(lane == 0, edges[0], jnp.where(d_ym > kf, ym - c, 0.0))
        total = total + jnp.where(lane == LANES - 1, edges[1], jnp.where(d_yp > kf, yp - c, 0.0))
        s = c + jnp.where(d_at > kf, NU_COEF * total, 0.0)
        stepped[k0 : k0 + some] = s
        rows = pl.ds(k0, some)
        sends.append(
            pltpu.make_async_copy(stepped.at[rows], stepped_hbm.at[rows], sems.at[len(sends)])
        )
        sends[-1].start()
        done = s.reshape(some, bx_n, SUB, LANES)
        halves = []
        for p in range(0, some, 2):
            halves += list(join_levels(done[p], done[p + 1]))
        out = swap_granules(jnp.concatenate(halves, axis=0))
        for q in range(some):
            kp = k0 // 2 + q // 2
            for bx in range(bx_n):
                g = (bx * 2 + q % 2) * SUB
                blocks[g : g + SUB, kp * LANES : (kp + 1) * LANES] = out[q * bx_n + bx]
    n = depth.shape[1]
    diagonal = iota((n, n), 0) == iota((n, n), 1)
    depth_col = jnp.sum(
        jnp.where(diagonal, jnp.broadcast_to(depth, (n, n)), 0.0), axis=1, keepdims=True
    )
    wet = (iota((n, width), 1) // HALF).astype(f32) < depth_col
    marked = jnp.where(wet, blocks[...], DRY).astype(bf16)
    taken = jnp.sum(sel[...].astype(f32), axis=1, keepdims=True) > 0
    chosen = jnp.dot(sel[...], marked, preferred_element_type=f32)
    chosen = jnp.where(taken, chosen, DRY).astype(bf16)
    cap = packed[0].shape[0]
    for i, chunk in enumerate(packed):
        chunk[:, :width] = chosen[i * cap : (i + 1) * cap]
        chunk[:, width:] = tail[i * cap : (i + 1) * cap]
    for send in sends:
        send.wait()


def clear_kernel(n_gy, c, above, buf, *rest):
    sent, (passed, sems, out_sems) = rest[:n_gy], rest[n_gy:]
    cap = passed.shape[1]
    width = above.shape[1]
    me = lax.axis_index("gy")
    chunks = [jnp.bitwise_xor(me, i) * cap for i in range(n_gy)]
    loads = [
        pltpu.make_async_copy(c.at[pl.ds(r, cap)], buf.at[i], sems.at[i])
        for i, r in enumerate(chunks)
    ]
    sends = [pltpu.make_async_copy(passed.at[i], sent[i], out_sems.at[i]) for i in range(n_gy)]
    for load in loads:
        load.start()
    low = iota((cap, LANES), 1) < HALF
    spans = [slice(v * LANES, (v + 1) * LANES) for v in range(width // LANES)]
    for i in range(n_gy):
        loads[i].wait()
        a = [ATTEN_WATER + ATTEN_CHL * buf[i, :, 0, at] for at in spans]
        both = [x + pltpu.roll(x, HALF, 1) for x in a]
        carry = jnp.zeros((cap, LANES), f32)
        sums = []
        for x, y in zip(a, both):
            sums.append(carry + jnp.where(low, x, y))
            carry = carry + y
        left = [jnp.exp(-x) for x in sums]
        before = [jnp.ones((cap, LANES), f32)] + left[:-1]
        prev = [pltpu.roll(jnp.where(low, x, y), HALF, 1) for x, y in zip(left, before)]
        for at, x, y in zip(spans, prev, left):
            above[i * cap : (i + 1) * cap, at] = x
            passed[i, :, at] = (x - y).astype(bf16)
        sends[i].start()
    for send in sends:
        send.wait()


def spread_tail(arrived, rows, width):
    tail = arrived[rows, width:].astype(f32)
    low = iota(tail.shape, 1) < HALF
    turned = pltpu.roll(tail, HALF, 1)
    return jnp.where(low, tail, turned), jnp.where(low, turned, tail)


def growth_kernel(n_gy, above, c, *rest):
    came, (arrived, counts_out, weight, part) = rest[:n_gy], rest[n_gy:]
    chunks, group, tracers, width = c.shape
    for i, chunk in enumerate(came):
        arrived[i * group : (i + 1) * group, :] = chunk[...]
    spans = [slice(v * LANES, (v + 1) * LANES) for v in range(width // LANES)]

    def weigh(i):
        rows = pl.ds(pl.multiple_of(i * group, group), group)
        _, light = spread_tail(arrived, rows, width)
        sent = [arrived[rows, at].astype(f32) for at in spans]
        wet = [x < WET for x in sent]
        ones = [jnp.where(x, 1.0 / HALF, 0.0) for x in wet]
        count = jnp.sum(functools.reduce(jnp.add, ones), axis=1, keepdims=True)
        count = jnp.broadcast_to(count, (group, LANES))
        counts_out[rows, :] = count
        tops = [light * above[rows, at] for at in spans]
        temp = [jnp.exp(GROWTH_TEMP * x) for x in sent]
        rest = [1.0 / (x + 1.0) for x in tops]
        for v in range(len(spans)):
            g = STEP_DT * (temp[v] * (tops[v] * rest[v]))
            weight[v, rows, :] = jnp.where(wet[v], g, 0.0)
        return count

    def gather(i, sums):
        r = pl.multiple_of(i * group, group)
        sums = list(sums)
        for v, at in enumerate(spans):
            for s in range(group):
                sums[s % 8] = sums[s % 8] + row_of(weight, v, r + s) * c[i, s, :, at]
        return sums

    def one(i, carry):
        sums = gather(i - 1, carry[:-1])
        return (*sums, carry[-1] + weigh(i))

    start = (*[jnp.zeros((tracers, LANES), f32)] * 8, weigh(0))
    *sums, counts = lax.fori_loop(1, chunks, one, start)
    sums = gather(chunks - 1, sums)
    total = functools.reduce(jnp.add, sums)
    total = total + pltpu.roll(total, HALF, 1)
    wet = jnp.broadcast_to(jnp.sum(counts, axis=0, keepdims=True), (tracers, LANES))
    line = jnp.where(iota((tracers, LANES), 1) < HALF, total, wet)
    part[...] = jnp.broadcast_to(line[None], part.shape)


def mixing_kernel(arrived, counts, mix):
    steps, slots, _ = mix.shape
    width = steps * LANES
    group = 16
    half = (iota((group, LANES), 1) // HALF).astype(f32)
    low = iota((group, LANES), 1) < HALF
    spans = [slice(v * LANES, (v + 1) * LANES) for v in range(steps)]

    def one(i, carry):
        rows = pl.ds(pl.multiple_of(i * group, group), group)
        amb, _ = spread_tail(arrived, rows, width)
        count = counts[rows, :]
        here = [arrived[rows, at].astype(f32) for at in spans]
        below = [
            pltpu.roll(jnp.where(low, y, x), HALF, 1) for x, y in zip(here, here[1:] + here[-1:])
        ]
        bend = [jnp.tanh(x - y) for x, y in zip(here, below)]
        for v in range(steps):
            m = (amb * (1.0 + 0.5 * bend[v])).astype(bf16).astype(f32)
            mix[v, rows, :] = jnp.where(half + float(2 * v + 1) < count, STEP_DT * m, 0.0)
        return carry

    lax.fori_loop(0, slots // group, one, 0)


def final_kernel(
    cap, parts, counts, weight, mix, rates_hbm, c, out, done, buf, rates, reactions, mix_up, mixed,
    sems, out_sems, rates_sem,
):
    chunks, group, tracers, width = buf.shape
    me = lax.axis_index("gy")
    rates_load = pltpu.make_async_copy(rates_hbm, rates, rates_sem)
    rates_load.start()

    def load(i):
        at = i * group
        r = jnp.bitwise_xor(me, at // cap) * cap + at % cap
        return c.at[pl.ds(r, group)], buf.at[i], out.at[pl.ds(r, group)]

    def start(i):
        source, kept, _ = load(i)
        pltpu.make_async_copy(source, kept, sems.at[i]).start()

    for i in range(AHEAD):
        start(i)
    rates_load.wait()
    n_rows = group * tracers
    lane = iota((tracers, LANES), 1)
    steps = width // LANES
    spans = [slice(v * LANES, (v + 1) * LANES) for v in range(steps)]

    total = jnp.sum(parts[...], axis=0)
    grown = jnp.sum(jnp.where(lane < HALF, total, 0.0), axis=1, keepdims=True)
    cells = HALF * total[:, LANES - 1 :]
    change = jnp.zeros((tracers, LANES), f32)
    for s in range(tracers):
        change = change + rates[:, s : s + 1] * jnp.broadcast_to(
            grown[s : s + 1, :], (tracers, LANES)
        )
    move = (-change / jnp.maximum(cells, 1.0))[None]
    i_row = iota((n_rows, tracers), 0) % tracers == iota((n_rows, tracers), 1)
    j_col = iota((tracers, n_rows), 1) % tracers == iota((tracers, n_rows), 0)
    spread = jnp.dot(i_row.astype(f32), rates[...], preferred_element_type=f32)
    spread = jnp.dot(spread, j_col.astype(f32), preferred_element_type=f32)
    one_slot = iota((n_rows, n_rows), 0) // tracers == iota((n_rows, n_rows), 1) // tracers
    reactions[...] = jnp.where(one_slot, spread, 0.0).astype(bf16)

    half = (iota((group, LANES), 1) // HALF).astype(f32)
    low = iota((group, LANES), 1) < HALF
    low3 = iota((4, tracers, LANES), 2) < HALF

    def one(i, carry):
        r = pl.multiple_of(i * group, group)
        rows = pl.ds(r, group)

        @pl.when(i + AHEAD < chunks)
        def _():
            start(i + AHEAD)

        source, kept_at, goes = load(i)
        pltpu.make_async_copy(source, kept_at, sems.at[i]).wait()
        count = counts[rows, :]
        kept = [mix[v, rows, :] for v in range(steps)]
        zero = jnp.zeros_like(kept[0])
        for v, (x, y) in enumerate(zip(kept, [zero] + kept[:-1])):
            mix_up[v] = pltpu.roll(jnp.where(low, x, y), HALF, 1)
        mixed[...] = jnp.dot(
            reactions[...], buf[i].reshape(n_rows, width).astype(bf16), preferred_element_type=f32
        )

        spare = count - half
        for s0 in range(0, group, 4):
            some = range(s0, s0 + 4)
            left = jnp.stack(
                [jnp.broadcast_to(spare[s : s + 1, :], (tracers, LANES)) for s in some]
            )
            at_v = lambda v: buf[i, s0 : s0 + 4, :, spans[min(v, steps - 1)]]
            stacked = lambda ref, v, r0: jnp.stack([row_of(ref, v, r0 + s) for s in some])
            turn = lambda x, y: pltpu.roll(jnp.where(low3, y, x), HALF, 2)
            xs = [at_v(v) for v in range(DEEP + 1)]
            turns = [turn(xs[v], xs[v + 1]) for v in range(DEEP)]
            before = pltpu.roll(xs[0], HALF, 2)
            for v, at in enumerate(spans):
                xs.append(at_v(v + DEEP + 1))
                turns.append(turn(xs[DEEP], xs[DEEP + 1]))
                x, z = xs.pop(0), turns.pop(0)
                m = mixed[s0 * tracers : (s0 + 4) * tracers, at].reshape(4, tracers, LANES)
                flux = stacked(mix, v, r) * (z - x) - stacked(mix_up, v, 0) * (x - before)
                y = x + (flux + stacked(weight, v, r) * m)
                buf[i, s0 : s0 + 4, :, at] = y + jnp.where(left > float(2 * v), move, 0.0)
                before = z
        pltpu.make_async_copy(kept_at, goes, out_sems.at[i]).start()
        return carry

    lax.fori_loop(0, chunks, one, 0)
    done[...] = move[0]
    for i in range(chunks):
        _, kept_at, goes = load(i)
        pltpu.make_async_copy(kept_at, goes, out_sems.at[i]).wait()


def warm_kernel(bx_n, by_n, n_gy, holder, light, flags, tally, stepped, _, *rest):
    returned, (out_hbm, blocks, out, sems) = rest[:n_gy], rest[n_gy:]
    levels, nx, ny = stepped.shape
    cap = returned[0].shape[0]
    n = bx_n * by_n
    _, _, own_col, rank_col = ranks(holder)
    turn = jnp.bitwise_xor(own_col.astype(jnp.int32), lax.axis_index("gy")).astype(f32)
    to_col = turn * cap + rank_col
    sel_t = (iota((n, n_gy * cap), 1).astype(f32) == to_col).astype(bf16)
    got = jnp.concatenate([r[...] for r in returned], axis=0)
    blocks[...] = jnp.dot(sel_t, got, preferred_element_type=f32)
    depth = (flags[...] * tally[...]).astype(f32)
    d = depth_rows(depth, by_n)
    d_at = jnp.concatenate(
        [jnp.broadcast_to(d[bx : bx + 1], (SUB, LANES)) for bx in range(bx_n)], axis=0
    )
    scale = WARMING_SCALE * light[...].astype(f32)
    sends = []
    for k0 in range(0, levels, WARM_BATCH):
        halves = []
        for q in range(WARM_BATCH):
            kp = k0 // 2 + q // 2
            for bx in range(bx_n):
                g = (bx * 2 + q % 2) * SUB
                halves.append(blocks[g : g + SUB, kp * LANES : (kp + 1) * LANES])
        swapped = swap_granules(jnp.stack(halves))
        for p in range(WARM_BATCH // 2):
            lo = swapped[2 * p * bx_n : (2 * p + 1) * bx_n]
            hi = swapped[(2 * p + 1) * bx_n : (2 * p + 2) * bx_n]
            for e, took in enumerate(join_levels(lo, hi)):
                k = k0 + 2 * p + e
                out[k] = stepped[k] + jnp.where(d_at > float(k), scale * took.reshape(nx, ny), 0.0)
        rows = pl.ds(k0, WARM_BATCH)
        sends.append(pltpu.make_async_copy(out.at[rows], out_hbm.at[rows], sems.at[len(sends)]))
        sends[-1].start()
    for send in sends:
        send.wait()


def vmem(n):
    return [pl.BlockSpec(memory_space=pltpu.VMEM)] * n


def shaped(shape, dtype):
    return jax.ShapeDtypeStruct(shape, dtype)


def params():
    return pltpu.CompilerParams(vmem_limit_bytes=20 << 20)


def in_hbm(x):
    return pltpu.with_memory_space_constraint(x, pltpu.HBM)


def on_device(
    thermal_anomaly,
    ambient_diffusion,
    solar_light,
    sea_tile_flags,
    flooded_layer_tally,
    tile_holder_rank,
    solute_amounts,
    reaction_rates,
):
    levels, nx, ny = thermal_anomaly.shape
    bx_n, by_n = nx // 8, ny // 8
    n_blocks = bx_n * by_n
    slots, tracers, width = solute_amounts.shape[2:]
    n_gy = lax.axis_size("gy")
    n_all = n_gy * lax.axis_size("gx")
    cap = slots // n_gy
    flags = sea_tile_flags.reshape(1, n_blocks)
    tally = flooded_layer_tally.reshape(1, n_blocks)
    holder = tile_holder_rank.reshape(1, n_blocks)
    amounts = in_hbm(solute_amounts.reshape(slots, tracers, width))

    sources = [thermal_anomaly, flags, tally, ambient_diffusion, solar_light, holder]
    x1, x2, y1, y2, *held = pl.pallas_call(
        functools.partial(edges_kernel, bx_n, by_n),
        out_shape=[shaped((levels + SUB, LANES), f32)] * 2
        + [shaped((2 * SUB, LANES), f32)] * 2
        + [pltpu.VMEM(x.shape, x.dtype) for x in sources],
        in_specs=[pl.BlockSpec(memory_space=pltpu.HBM)] * len(sources),
        out_specs=vmem(4 + len(sources)),
        scratch_shapes=[pltpu.SemaphoreType.DMA((len(sources),))],
        compiler_params=params(),
        name="edges",
    )(*[in_hbm(x) for x in sources])
    thermal, flags, tally, ambient, light, holder = held

    def traded(x, axis, first):
        count = lax.axis_size(axis)
        pairs = [(i, i + 1) for i in range(first, count - 1, 2)]
        return lax.ppermute(x, axis, pairs + [(j, i) for i, j in pairs])

    far_y2 = traded(y2, "gy", 1)
    far_x2 = traded(x2, "gx", 1)
    far_y1 = traded(y1, "gy", 0)
    far_x1 = traded(x1, "gx", 0)

    sel, tail = pl.pallas_call(
        functools.partial(slots_kernel, bx_n, by_n, cap),
        out_shape=[
            shaped((slots, n_blocks), bf16),
            shaped((slots, LANES), bf16),
        ],
        in_specs=vmem(3),
        out_specs=vmem(2),
        compiler_params=params(),
        name="slots",
    )(ambient, light, holder)

    group = min(16, cap)
    steps = slots // group
    buffers = [
        pltpu.VMEM((steps, group, tracers, width), f32),
        pltpu.SemaphoreType.DMA((steps,)),
    ]
    any_hbm = pl.BlockSpec(memory_space=pltpu.HBM)
    above, held_amounts, *passed = pl.pallas_call(
        functools.partial(clear_kernel, n_gy),
        out_shape=[
            pltpu.VMEM((slots, width), f32),
            pltpu.VMEM((n_gy, cap, tracers, width), f32),
        ]
        + [pltpu.HBM((cap, width), bf16)] * n_gy,
        in_specs=[any_hbm],
        out_specs=vmem(2) + [any_hbm] * n_gy,
        scratch_shapes=[
            pltpu.VMEM((n_gy, cap, width), bf16),
            pltpu.SemaphoreType.DMA((n_gy,)),
            pltpu.SemaphoreType.DMA((n_gy,)),
        ],
        compiler_params=params(),
        name="clear",
    )(amounts)

    stepped, *packed = pl.pallas_call(
        functools.partial(stencil_kernel, bx_n, by_n),
        out_shape=[pltpu.HBM((levels, nx, ny), f32)]
        + [shaped((cap, width + LANES), bf16)] * n_gy,
        in_specs=vmem(11),
        out_specs=[any_hbm] + vmem(n_gy),
        scratch_shapes=[pltpu.VMEM((n_blocks, width), f32)]
        + [pltpu.VMEM((levels + SUB, LANES), f32)] * 2
        + [pltpu.VMEM((levels, nx, ny), f32), pltpu.SemaphoreType.DMA((levels // BATCH,))],
        compiler_params=params(),
        name="stencil",
    )(thermal, flags, tally, far_x1, far_x2, far_y1, far_y2, y1, y2, sel, tail)

    def swapped(x, d):
        return lax.ppermute(x, "gy", [(i, i ^ d) for i in range(n_gy)])

    came = [packed[0]]
    for d in range(1, n_gy):
        came.append(swapped(packed[d], d))

    arrived, counts, weight, part = pl.pallas_call(
        functools.partial(growth_kernel, n_gy),
        out_shape=[
            shaped((slots, width + LANES), bf16),
            shaped((slots, LANES), f32),
            shaped((width // LANES, slots, LANES), f32),
            shaped((n_all, tracers, LANES), f32),
        ],
        in_specs=vmem(2 + n_gy),
        out_specs=vmem(4),
        compiler_params=params(),
        name="growth",
    )(
        pltpu.with_memory_space_constraint(above, pltpu.VMEM),
        pltpu.with_memory_space_constraint(held_amounts, pltpu.VMEM),
        *came,
    )

    parts = lax.all_to_all(part, ("gx", "gy"), 0, 0, tiled=True)
    returned = [passed[0]]
    for d in range(1, n_gy):
        returned.append(swapped(passed[d], d))

    mix = pl.pallas_call(
        mixing_kernel,
        out_shape=shaped((width // LANES, slots, LANES), f32),
        in_specs=vmem(2),
        out_specs=pl.BlockSpec(memory_space=pltpu.VMEM),
        compiler_params=params(),
        name="mixing",
    )(arrived, counts)
    by_lane = pltpu.VMEM((width // LANES, group, LANES), f32)
    out, done = pl.pallas_call(
        functools.partial(final_kernel, cap),
        out_shape=[shaped((slots, tracers, width), f32), shaped((tracers, LANES), f32)],
        in_specs=vmem(4) + [any_hbm] * 2,
        out_specs=[any_hbm] + vmem(1),
        scratch_shapes=[
            buffers[0],
            pltpu.VMEM((tracers, tracers), f32),
            pltpu.VMEM((group * tracers, group * tracers), bf16),
            by_lane,
            pltpu.VMEM((group * tracers, width), f32),
            buffers[1],
            buffers[1],
            pltpu.SemaphoreType.DMA,
        ],
        compiler_params=params(),
        name="final",
    )(parts, counts, weight, mix, in_hbm(reaction_rates), amounts)

    thermal_final = pl.pallas_call(
        functools.partial(warm_kernel, bx_n, by_n, n_gy),
        out_shape=shaped((levels, nx, ny), f32),
        in_specs=vmem(6 + n_gy),
        out_specs=any_hbm,
        scratch_shapes=[
            pltpu.VMEM((n_blocks, width), f32),
            pltpu.VMEM((levels, nx, ny), f32),
            pltpu.SemaphoreType.DMA((levels // WARM_BATCH,)),
        ],
        compiler_params=params(),
        name="warm",
    )(holder, light, flags, tally, stepped, done, *returned)
    return thermal_final, out.reshape(solute_amounts.shape)


def solution(mesh):
    return jax.shard_map(
        on_device,
        mesh=mesh,
        in_specs=(
            P(None, "gx", "gy"),
            P("gx", "gy"),
            P("gx", "gy"),
            P("gx", "gy", None),
            P("gx", "gy", None),
            P("gx", "gy", None, None),
            P("gx", "gy", None, None, None),
            P(),
        ),
        out_specs=(P(None, "gx", "gy"), P("gx", "gy", None, None, None)),
        check_vma=False,
    )
```
